1024 devices in a mesh: gx: 32 (over z), gy: 32 (over x, y, core).
Axes of the slice: x: 4, y: 4, z: 32, core: 2. Of those that a mesh axis runs over, the one named last changes fastest.
Arguments:
- conductivity: float32 [1024, 1024, 128], P('gx', 'gy'), may hold values from 0.25 to 4
- source: float32 [1024, 1024, 128], P('gx', 'gy'), may hold values from -12 to 12
- initial: float32 [1024, 1024, 128], P('gx', 'gy'), may hold values from -3 to 3
Outputs:
- solution: float32 [1024, 1024, 128], P('gx', 'gy')
The draws below stay inside these ranges and needn't reach their ends.
All inputs are finite; a program needn't handle non-finite values.
Results may differ from the reference program's by a relative error of at most 0.0003.
Values sent between devices are 32-bit elements; how exact they have to be, the bound alone decides.
No kernel may reach another device: no remote copies, remote signals or barrier semaphores. Data moves between devices by JAX's collectives and lax.ppermute only.
A program may use at most 32 MiB of HBM per device.

```python
import math
import jax
import jax.numpy as jnp
from jax import lax

BS = 16
NU = 3
CG_ITERS = 32
NX = 1024
NY = 1024
NZ = 128
N_GX = 32
N_GY = 32


def draw_source(key, part):
    return 4.0 * jax.random.truncated_normal(key, -3.0, 3.0, (NX, NY, NZ), jnp.float32)


def level_of(key, dims, split, smallest, high):
    def one(dim, blocks):
        heights = jax.random.uniform(jax.random.fold_in(jax.random.fold_in(key, 6), dim), (blocks,), jnp.float32, smallest / len(split), high / len(split))
        return jnp.repeat(jnp.exp(heights), dims[dim] // blocks).reshape((-1,) + (1,) * (len(dims) - dim - 1))

    level = one(*split[0])
    for cut in split[1:]:
        level = level * one(*cut)
    return level


def bell_draw(own_key, dims, spread, reach, shards=(), kind=jnp.bfloat16):
    values = jax.random.normal(own_key, dims, jnp.float32) * spread
    if len(shards) > 0:
        values = level_of(own_key, dims, shards, -0.22, 0.18) * values
    return jnp.clip(values, min=-reach, max=reach).astype(kind)


def setup_inputs(seed: int = 0) -> dict:
    seeds = jax.random.split(jax.random.key(seed), 4)
    return {
        "conductivity": jnp.clip(jnp.exp(math.log(4.0) - 2.7725887 * jax.random.uniform(seeds[0], (NX, NY, NZ), jnp.float32) ** level_of(seeds[0], (NX, NY, NZ), ((0, 32), (1, 32)), -0.2, 0.2)), 0.25, 4.0),
        "source": draw_source(jax.random.fold_in(seeds[3], 71), 0),
        "initial": bell_draw(seeds[2], (NX, NY, NZ), 0.5, 3.0, ((0, 32), (1, 32)), jnp.float32),
    }


relax_weight = 0.8


def operate(padded, cond_pad):
    center_cond = cond_pad[1:-1, 1:-1]
    center = padded[1:-1, 1:-1]
    face_east = 0.5 * (center_cond + cond_pad[2:, 1:-1])
    face_west = 0.5 * (center_cond + cond_pad[:-2, 1:-1])
    face_north = 0.5 * (center_cond + cond_pad[1:-1, 2:])
    face_south = 0.5 * (center_cond + cond_pad[1:-1, :-2])
    between = 0.5 * (center_cond[:, :, 1:] + center_cond[:, :, :-1])
    zero_plane = jnp.zeros(center.shape[:2] + (1,), center.dtype)
    face_up = jnp.concatenate([between, zero_plane], 2)
    face_down = jnp.concatenate([zero_plane, between], 2)
    value_up = jnp.concatenate([center[:, :, 1:], zero_plane], 2)
    value_down = jnp.concatenate([zero_plane, center[:, :, :-1]], 2)
    diagonal = face_east + face_west + face_north + face_south + face_up + face_down
    neighbor_sum = (face_east * padded[2:, 1:-1] + face_west * padded[:-2, 1:-1]
                    + face_north * padded[1:-1, 2:] + face_south * padded[1:-1, :-2]
                    + face_up * value_up + face_down * value_down)
    return diagonal * center - neighbor_sum, diagonal, center_cond, center


def smooth_once(padded, cond_pad, source):
    applied, diagonal, center_cond, center = operate(padded, cond_pad)
    inside = center_cond > 0
    update = relax_weight * (source - applied) / jnp.where(inside, diagonal, 1.0)
    return jnp.where(inside, center + update, 0.0)


def coarse_apply(estimate, coarse_diag, flow_east, flow_north):
    edge_rows = jnp.zeros((1, estimate.shape[1]), estimate.dtype)
    edge_cols = jnp.zeros((estimate.shape[0], 1), estimate.dtype)
    ahead_x = jnp.concatenate([estimate[1:], edge_rows], 0)
    carried_x = flow_east * estimate
    behind_x = jnp.concatenate([edge_rows, carried_x[:-1]], 0)
    ahead_y = jnp.concatenate([estimate[:, 1:], edge_cols], 1)
    carried_y = flow_north * estimate
    behind_y = jnp.concatenate([edge_cols, carried_y[:, :-1]], 1)
    return coarse_diag * estimate - flow_east * ahead_x - behind_x - flow_north * ahead_y - behind_y


def coarse_solve(coarse_source, coarse_diag, flow_east, flow_north):
    def iterate_once(counter, carried):
        estimate, remainder, search, norm_now = carried
        product = coarse_apply(search, coarse_diag, flow_east, flow_north)
        alpha_step = norm_now / jnp.sum(search * product)
        estimate = estimate + alpha_step * search
        remainder = remainder - alpha_step * product
        norm_next = jnp.sum(remainder * remainder)
        search = remainder + (norm_next / norm_now) * search
        return estimate, remainder, search, norm_next

    start_state = (jnp.zeros_like(coarse_source), coarse_source, coarse_source,
                   jnp.sum(coarse_source * coarse_source))
    return lax.fori_loop(0, CG_ITERS, iterate_once, start_state)[0]


def reference(conductivity, source, initial):
    extent_x = 2 * BS
    extent_y = 2 * BS
    margins = ((1, 1), (1, 1), (0, 0))
    cond_pad = jnp.pad(conductivity, margins)
    starts = jnp.arange(N_GX, dtype=jnp.int32) * extent_x

    def sweep_all(iterate):
        padded = jnp.pad(iterate, margins)

        def one_slab(offset):
            return smooth_once(lax.dynamic_slice_in_dim(padded, offset, extent_x + 2, 0),
                               lax.dynamic_slice_in_dim(cond_pad, offset, extent_x + 2, 0),
                               lax.dynamic_slice_in_dim(source, offset, extent_x, 0))

        return lax.map(one_slab, starts).reshape(conductivity.shape)

    iterate = initial
    for repeat in range(NU):
        iterate = sweep_all(iterate)
    padded = jnp.pad(iterate, margins)

    def slab_residual(offset):
        applied = operate(lax.dynamic_slice_in_dim(padded, offset, extent_x + 2, 0),
                          lax.dynamic_slice_in_dim(cond_pad, offset, extent_x + 2, 0))[0]
        remainder = lax.dynamic_slice_in_dim(source, offset, extent_x, 0) - applied
        return jnp.sum(remainder.reshape(extent_x, N_GY, extent_y, -1), axis=(0, 2, 3))

    coarse_source = lax.map(slab_residual, starts)
    whole_x = conductivity.shape[0]
    high_x = jnp.pad(conductivity, ((0, 1), (0, 0), (0, 0)))
    plane = 0.5 * (conductivity[extent_x - 1::extent_x] + high_x[extent_x::extent_x])
    flow_east = jnp.sum(plane.reshape(N_GX, N_GY, extent_y, -1), axis=(2, 3))
    low_x = jnp.pad(conductivity, ((1, 0), (0, 0), (0, 0)))
    plane = 0.5 * (conductivity[0::extent_x] + low_x[0:whole_x:extent_x])
    flow_west = jnp.sum(plane.reshape(N_GX, N_GY, extent_y, -1), axis=(2, 3))
    high_y = jnp.pad(conductivity, ((0, 0), (0, 1), (0, 0)))
    plane = 0.5 * (conductivity[:, extent_y - 1::extent_y] + high_y[:, extent_y::extent_y])
    flow_north = jnp.sum(plane.reshape(N_GX, extent_x, N_GY, -1), axis=(1, 3))
    low_y = jnp.pad(conductivity, ((0, 0), (1, 0), (0, 0)))
    plane = 0.5 * (conductivity[:, 0::extent_y] + low_y[:, 0:conductivity.shape[1]:extent_y])
    flow_south = jnp.sum(plane.reshape(N_GX, extent_x, N_GY, -1), axis=(1, 3))
    coarse_diag = flow_east + flow_west + flow_north + flow_south
    correction = coarse_solve(coarse_source, coarse_diag, flow_east, flow_north)
    iterate = iterate + jnp.repeat(jnp.repeat(correction, extent_x, 0), extent_y, 1)[:, :, None]
    for repeat in range(NU):
        iterate = sweep_all(iterate)
    return iterate
```

```python
import functools
import jax
import jax.numpy as jnp
from jax import lax
from jax.experimental import pallas as pl
from jax.experimental.pallas import tpu as pltpu
from jax.sharding import PartitionSpec as P

NU = 3
CG_ITERS = 32


relax_weight = 0.8
REACH = 2 * NU
WIDTHS = (REACH, REACH - 1, REACH)
LANES = 128
TILE = 8


def ring_pairs(count, step):
    return [(i, i + step) for i in range(count) if 0 <= i + step < count]


def strip_rows(extent_x):
    rows = []
    for array, width in enumerate(WIDTHS):
        for plane in range(REACH - width, REACH + extent_x + width):
            beyond = max(REACH - plane, plane - (REACH + extent_x - 1), 0)
            if width - beyond > 0:
                rows.append((array, plane, width - beyond))
    return rows


def slab_plane(array, plane, extent_x):
    start = sum(WIDTHS[:array])
    if plane < REACH:
        return 0, start + plane - (REACH - WIDTHS[array])
    return 1, start + plane - (REACH + extent_x)


def strips_kernel(extent_x, low_refs, high_refs, slab_low_refs, slab_high_refs, up_ref, down_ref):
    at = 0
    for array, plane, rows in strip_rows(extent_x):
        if REACH <= plane < REACH + extent_x:
            low, high, where = low_refs[array], high_refs[array], plane - REACH
        else:
            side, where = slab_plane(array, plane, extent_x)
            low, high = slab_low_refs[side], slab_high_refs[side]
        up_ref[at : at + rows, :] = high[where, TILE - rows : TILE, :]
        down_ref[at : at + rows, :] = low[where, 0:rows, :]
        at += rows


def pack_strips(arrays, slabs):
    extent_x, extent_y = arrays[0].shape[:2]
    length = sum(rows for _, _, rows in strip_rows(extent_x))
    last = extent_y // TILE - 1

    def kernel(*refs):
        strips_kernel(extent_x, refs[0:3], refs[3:6], refs[6:8], refs[8:10], *refs[10:])

    def edge(array, block):
        return pl.BlockSpec((array.shape[0], TILE, LANES), lambda i: (0, block, 0))

    return pl.pallas_call(
        kernel,
        grid=(1,),
        in_specs=[edge(a, 0) for a in arrays]
        + [edge(a, last) for a in arrays]
        + [edge(a, 0) for a in slabs]
        + [edge(a, last) for a in slabs],
        out_specs=[pl.BlockSpec((length, LANES), lambda i: (0, 0))] * 2,
        out_shape=[jax.ShapeDtypeStruct((length, LANES), jnp.float32)] * 2,
        name="pack_strips",
    )(*arrays, *arrays, *slabs, *slabs)


def plane_rolls(values, axis):
    return pltpu.roll(values, values.shape[axis] - 1, axis), pltpu.roll(values, 1, axis)


def coefficients(cond, cond_next, face_west, lane):
    face_east = 0.5 * (cond + cond_next)
    face_north = 0.5 * (cond + plane_rolls(cond, 0)[0])
    face_south = plane_rolls(face_north, 0)[1]
    face_up = jnp.where(lane < LANES - 1, 0.5 * (cond + plane_rolls(cond, 1)[0]), 0.0)
    face_down = plane_rolls(face_up, 1)[1]
    diagonal = face_east + face_west + face_north + face_south + face_up + face_down
    scale = jnp.where(cond > 0, relax_weight / diagonal, 0.0)
    return face_east, face_north, face_south, face_up, face_down, scale


def smooth_plane(value, value_next, value_before, faces, source):
    face_east, face_west, face_north, face_south, face_up, face_down, scale = faces
    north, south = plane_rolls(value, 0)
    up, down = plane_rolls(value, 1)
    near = (
        (face_east * value_next + face_west * value_before)
        + (face_north * north + face_south * south)
        + (face_up * up + face_down * down)
    )
    return (1.0 - relax_weight) * value + scale * (source + near)


def sweep(first, last, source_of, value_ref, result_ref, faces_of):
    def one(plane, carried):
        before, value, face_west = carried
        value_next = value_ref[plane + 1]
        face_east, rest = faces_of(plane)
        result_ref[plane] = smooth_plane(
            value, value_next, before, (face_east, face_west, *rest), source_of(plane)
        )
        return value, value_next, face_east

    return one


def assemble(refs, slab_refs, ext_refs, sems, arrays):
    copies = []
    for array in arrays:
        ref, ext, width = refs[array], ext_refs[array], WIDTHS[array]
        extent_x, extent_y = ref.shape[0], ref.shape[1]
        rows = pl.ds(TILE, extent_y)
        start = sum(WIDTHS[:array])
        moves = [
            (ref, ext.at[pl.ds(REACH, extent_x), rows]),
            (slab_refs[0].at[pl.ds(start, width)], ext.at[pl.ds(REACH - width, width), rows]),
            (slab_refs[1].at[pl.ds(start, width)], ext.at[pl.ds(REACH + extent_x, width), rows]),
        ]
        for source, target in moves:
            copy = pltpu.make_async_copy(source, target, sems.at[len(copies)])
            copy.start()
            copies.append(copy)
    return copies


def clear_rims(ext_refs, extent_x, extent_y, arrays):
    for array in arrays:
        ext = ext_refs[array]
        planes = ext.shape[0]
        zeros = jnp.zeros((planes, TILE, LANES), jnp.float32)
        ext[:, 0:TILE, :] = zeros
        ext[:, TILE + extent_y : 2 * TILE + extent_y, :] = zeros
        width = WIDTHS[array]
        for plane in range(REACH - width):
            for side in (plane, planes - 1 - plane):
                ext[side, TILE : TILE + extent_y, :] = jnp.zeros((extent_y, LANES), jnp.float32)


def place_strips(low_ref, high_ref, ext_refs, extent_x, extent_y):
    at = 0
    for array, plane, rows in strip_rows(extent_x):
        ext = ext_refs[array]
        ext[plane, TILE - rows : TILE, :] = low_ref[at : at + rows, :]
        ext[plane, TILE + extent_y : TILE + extent_y + rows, :] = high_ref[at : at + rows, :]
        at += rows


def before_kernel(
    index_ref, cond_in, source_in, value_in, slab_low, slab_high, strip_low, strip_high,
    row_ref, value_out, cond_ext, source_ext, value_ext, other, face_x, face_n, face_s, face_u,
    face_d, scales, sems,
):
    extent_x, extent_y = cond_in.shape[0], cond_in.shape[1]
    planes = extent_x + 2 * REACH
    exts = (cond_ext, source_ext, value_ext)
    copies = assemble(
        (cond_in, source_in, value_in), (slab_low, slab_high), exts, sems, (0, 1, 2)
    )
    clear_rims(exts, extent_x, extent_y, (0, 1, 2))
    place_strips(strip_low, strip_high, exts, extent_x, extent_y)
    for copy in copies:
        copy.wait()
    shape = (extent_y + 2 * TILE, LANES)
    lane = lax.broadcasted_iota(jnp.int32, shape, 1)

    def first(plane, carried):
        before, value, face_west = carried
        value_next = value_ext[plane + 1]
        made = coefficients(cond_ext[plane], cond_ext[plane + 1], face_west, lane)
        for ref, part in zip((face_x, face_n, face_s, face_u, face_d, scales), made):
            ref[plane] = part
        other[plane] = smooth_plane(
            value, value_next, before, (made[0], face_west, *made[1:]), source_ext[plane]
        )
        return value, value_next, made[0]

    face_first = 0.5 * (cond_ext[0] + cond_ext[1])
    lax.fori_loop(1, planes - 1, first, (value_ext[0], value_ext[1], face_first))

    def repeat(low, value_ref, result_ref, shift):
        def one(plane, carried):
            before, value, face_west = carried
            value_next = value_ref[plane + 1]
            face_east = face_x[plane]
            faces = (
                face_east, face_west, face_n[plane], face_s[plane], face_u[plane], face_d[plane],
                scales[plane],
            )
            result_ref[plane - shift] = smooth_plane(
                value, value_next, before, faces, source_ext[plane]
            )
            return value, value_next, face_east

        lax.fori_loop(
            low, planes - low, one, (value_ref[low - 1], value_ref[low], face_x[low - 1])
        )

    repeat(2, other, value_ext, 0)
    repeat(3, value_ext, value_out, NU)

    inner = slice(TILE, TILE + extent_y)
    low_x, high_x = REACH, REACH + extent_x - 1

    def out_x(plane):
        return value_out[plane - NU, inner, :]

    east = face_x[high_x, inner, :]
    west = face_x[low_x - 1, inner, :]
    net = east * (out_x(high_x + 1) - out_x(high_x)) + west * (out_x(low_x - 1) - out_x(low_x))
    edge_low, edge_high = slice(0, 2 * TILE), slice(extent_y, extent_y + 2 * TILE)
    zero = jnp.zeros((extent_y, LANES), jnp.float32)
    zero_edge = jnp.zeros((2 * TILE, LANES), jnp.float32)

    def along(plane, carried):
        sources, flow_low, flow_high, face_low, face_high = carried
        sources = sources + source_ext[plane, inner, :]
        value = value_out[plane - NU, edge_low, :]
        face = face_n[plane, edge_low, :]
        flow_low = flow_low + face * (plane_rolls(value, 0)[0] - value)
        face_low = face_low + face
        value = value_out[plane - NU, edge_high, :]
        face = face_n[plane, edge_high, :]
        flow_high = flow_high + face * (plane_rolls(value, 0)[0] - value)
        face_high = face_high + face
        return sources, flow_low, flow_high, face_low, face_high

    sources, flow_low, flow_high, face_low, face_high = lax.fori_loop(
        low_x, high_x + 1, along, (zero, zero_edge, zero_edge, zero_edge, zero_edge)
    )
    edge_row = lax.broadcasted_iota(jnp.int32, zero_edge.shape, 0) == TILE - 1

    def whole(values):
        return jnp.sum(jnp.sum(values, axis=0, keepdims=True), axis=1, keepdims=True)

    def face_sum(values):
        return whole(jnp.where(edge_row, values, 0.0))

    flow_north, flow_south = face_sum(face_high), face_sum(face_low)
    flow_east, flow_west = whole(east), whole(west)
    residual = whole(sources + net) + face_sum(flow_high) - face_sum(flow_low)
    diag = flow_east + flow_west + flow_north + flow_south
    own = lax.broadcasted_iota(jnp.int32, row_ref.shape, 1)
    count = LANES // 4
    place = own - index_ref[1]
    row_ref[...] = jnp.where(
        place == 0,
        residual,
        jnp.where(
            place == count,
            diag,
            jnp.where(
                place == 2 * count, flow_east, jnp.where(place == 3 * count, flow_north, 0.0)
            ),
        ),
    )


def total(values):
    folded = values[0:8] + values[8:16] + values[16:24] + values[24:32]
    return jnp.sum(jnp.sum(folded, axis=1, keepdims=True), axis=0, keepdims=True)


def shifted(values):
    return (
        pltpu.roll(values, 31, 0),
        pltpu.roll(values, 1, 0),
        pltpu.roll(values, 127, 1),
        pltpu.roll(values, 1, 1),
    )


def coarse_solve(packed, count_x, count_y):
    row = lax.broadcasted_iota(jnp.int32, packed.shape, 0)
    lane = lax.broadcasted_iota(jnp.int32, packed.shape, 1)
    inside = lane < 32
    start = jnp.where(inside, packed, 0.0)
    diag = jnp.where(inside, pltpu.roll(packed, 96, 1), 0.0)
    east = jnp.where(inside & (row < count_x - 1), pltpu.roll(packed, 64, 1), 0.0)
    north = jnp.where(lane < count_y - 1, pltpu.roll(packed, 32, 1), 0.0)
    west = pltpu.roll(east, 1, 0)
    south = pltpu.roll(north, 1, 1)

    def iterate_once(counter, carried):
        estimate, remainder, search, ahead_x, behind_x, ahead_y, behind_y, norm_now = carried
        product = (
            diag * search
            - (east * ahead_x + west * behind_x)
            - (north * ahead_y + south * behind_y)
        )
        alpha_step = norm_now / total(search * product)
        estimate = estimate + alpha_step * search
        remainder = remainder - alpha_step * product
        moved = shifted(remainder)
        norm_next = total(remainder * remainder)
        beta = norm_next / norm_now
        search = remainder + beta * search
        around = [
            m + beta * a for m, a in zip(moved, (ahead_x, behind_x, ahead_y, behind_y))
        ]
        return (estimate, remainder, search, *around, norm_next)

    state = (jnp.zeros_like(start), start, start, *shifted(start), total(start * start))
    return lax.fori_loop(0, CG_ITERS, iterate_once, state)[0]


def after_kernel(
    counts, index_ref, packed_ref, cond_in, source_in, slab_low, slab_high, strip_low, strip_high, value_in,
    out_ref, cond_ext, source_ext, value_ext, other, face_x, face_n, face_s, face_u, face_d,
    scales, sems,
):
    extent_x, extent_y = cond_in.shape[0], cond_in.shape[1]
    planes = extent_x + 2 * REACH
    exts = (cond_ext, source_ext)
    copies = assemble((cond_in, source_in), (slab_low, slab_high), exts, sems, (0, 1))
    copy = pltpu.make_async_copy(value_in, value_ext.at[pl.ds(NU, planes - 2 * NU)], sems.at[6])
    copy.start()
    copies.append(copy)
    estimate = coarse_solve(packed_ref[...], *counts)
    clear_rims(exts, extent_x, extent_y, (0, 1))
    at = 0
    for array, plane, rows in strip_rows(extent_x):
        if array < 2:
            ext = exts[array]
            ext[plane, TILE - rows : TILE, :] = strip_low[at : at + rows, :]
            ext[plane, TILE + extent_y : TILE + extent_y + rows, :] = strip_high[at : at + rows, :]
        at += rows
    shape = (extent_y + 2 * TILE, LANES)
    row = lax.broadcasted_iota(jnp.int32, shape, 0)
    lane = lax.broadcasted_iota(jnp.int32, shape, 1)
    brick_row = lax.broadcasted_iota(jnp.int32, estimate.shape, 0)
    brick_lane = lax.broadcasted_iota(jnp.int32, estimate.shape, 1)

    def share(step_x, step_y):
        mine = (brick_row == index_ref[0] + step_x) & (brick_lane == index_ref[1] + step_y)
        return total(jnp.where(mine, estimate, 0.0))

    def column(step_x):
        low, own, high = (share(step_x, step) for step in (-1, 0, 1))
        return jnp.where(row < TILE, low, jnp.where(row < TILE + extent_y, own, high))

    lifts = [column(step) for step in (-1, 0, 1)]
    for copy in copies:
        copy.wait()

    def lift(low, high, amount):
        def one(plane, carried):
            inside = cond_ext[plane] > 0
            value_ext[plane] = value_ext[plane] + jnp.where(inside, amount, 0.0)
            return carried

        lax.fori_loop(low, high, one, 0)

    lift(NU, REACH, lifts[0])
    lift(REACH, REACH + extent_x, lifts[1])
    lift(REACH + extent_x, planes - NU, lifts[2])

    def first(plane, carried):
        before, value, face_west = carried
        value_next = value_ext[plane + 1]
        made = coefficients(cond_ext[plane], cond_ext[plane + 1], face_west, lane)
        for ref, part in zip((face_x, face_n, face_s, face_u, face_d, scales), made):
            ref[plane] = part
        other[plane] = smooth_plane(
            value, value_next, before, (made[0], face_west, *made[1:]), source_ext[plane]
        )
        return value, value_next, made[0]

    low = NU + 1
    face_first = 0.5 * (cond_ext[low - 1] + cond_ext[low])
    face_x[low - 1] = face_first
    lax.fori_loop(low, planes - low, first, (value_ext[low - 1], value_ext[low], face_first))

    def repeat(low, value_ref, store):
        def one(plane, carried):
            before, value, face_west = carried
            value_next = value_ref[plane + 1]
            face_east = face_x[plane]
            faces = (
                face_east, face_west, face_n[plane], face_s[plane], face_u[plane], face_d[plane],
                scales[plane],
            )
            store(plane, smooth_plane(value, value_next, before, faces, source_ext[plane]))
            return value, value_next, face_east

        lax.fori_loop(
            low, planes - low, one, (value_ref[low - 1], value_ref[low], face_x[low - 1])
        )

    def keep(plane, value):
        value_ext[plane] = value

    def finish(plane, value):
        out_ref[plane - REACH] = value[TILE : TILE + extent_y]

    repeat(NU + 2, other, keep)
    repeat(NU + 3, value_ext, finish)


def spread(row, axis):
    count = lax.axis_size(axis)
    blocks = jnp.broadcast_to(row, (count, row.shape[1]))
    return lax.all_to_all(blocks, axis, 0, 0, tiled=True)


def body(conductivity, source, initial):
    arrays = (conductivity, source, initial)
    extent_x, extent_y = conductivity.shape[:2]
    count_x, count_y = lax.axis_size("gx"), lax.axis_size("gy")
    index = jnp.stack([lax.axis_index("gx"), lax.axis_index("gy")]).astype(jnp.int32)
    tails = jnp.concatenate([a[extent_x - w :] for a, w in zip(arrays, WIDTHS)], 0)
    heads = jnp.concatenate([a[:w] for a, w in zip(arrays, WIDTHS)], 0)
    slabs = (
        lax.ppermute(tails, "gx", ring_pairs(count_x, 1)),
        lax.ppermute(heads, "gx", ring_pairs(count_x, -1)),
    )
    up, down = pack_strips(arrays, slabs)
    strips = (
        lax.ppermute(up, "gy", ring_pairs(count_y, 1)),
        lax.ppermute(down, "gy", ring_pairs(count_y, -1)),
    )
    planes, rows = extent_x + 2 * REACH, extent_y + 2 * TILE
    scratch = [pltpu.VMEM((planes, rows, LANES), jnp.float32)] * 10
    smem = pl.BlockSpec(memory_space=pltpu.SMEM)
    vmem = pl.BlockSpec(memory_space=pltpu.VMEM)
    leave = pl.BlockSpec(memory_space=pl.ANY)
    row, smoothed = pl.pallas_call(
        before_kernel,
        in_specs=[smem] + [leave] * 5 + [vmem] * 2,
        out_specs=[vmem, vmem],
        out_shape=[
            jax.ShapeDtypeStruct((1, LANES), jnp.float32),
            jax.ShapeDtypeStruct((planes - 2 * NU, rows, LANES), jnp.float32),
        ],
        scratch_shapes=scratch + [pltpu.SemaphoreType.DMA((9,))],
        name="smooth_before",
    )(index, *arrays, *slabs, *strips)
    row = jnp.sum(spread(row, "gy"), axis=0, keepdims=True)
    packed = spread(row, "gx")
    packed = jnp.pad(packed, ((0, LANES // 4 - count_x), (0, 0)))
    return pl.pallas_call(
        functools.partial(after_kernel, (count_x, count_y)),
        in_specs=[smem, vmem] + [leave] * 4 + [vmem] * 2 + [leave],
        out_specs=vmem,
        out_shape=jax.ShapeDtypeStruct(conductivity.shape, jnp.float32),
        scratch_shapes=scratch + [pltpu.SemaphoreType.DMA((7,))],
        name="smooth_after",
    )(index, packed, conductivity, source, *slabs, *strips, smoothed)


def solution(mesh):
    return jax.shard_map(
        body,
        mesh=mesh,
        in_specs=(P("gx", "gy", None), P("gx", "gy", None), P("gx", "gy", None)),
        out_specs=P("gx", "gy", None),
        check_vma=False,
    )
```

```python
import jax
import jax.numpy as jnp
from jax import lax
from jax.experimental import pallas as pl
from jax.experimental.pallas import tpu as pltpu
from jax.sharding import PartitionSpec as P

NU = 3
CG_ITERS = 32


relax_weight = 0.8
REACH = 2 * NU
WIDTHS = (REACH, REACH - 1, REACH)
LANES = 128
TILE = 8
SIDE = 32


def ring_pairs(count, step):
    return [(i, i + step) for i in range(count) if 0 <= i + step < count]


def own_rows():
    return [(array, row) for array, width in enumerate(WIDTHS) for row in range(width)]


def corner_rows(extent_x):
    rows = []
    for array, width in enumerate(WIDTHS):
        for beyond in range(1, width):
            for plane in (REACH - beyond, REACH + extent_x - 1 + beyond):
                rows.append((array, plane, width - beyond))
    return rows


def slab_plane(array, plane, extent_x):
    start = sum(WIDTHS[:array])
    if plane < REACH:
        return 0, start + plane - (REACH - WIDTHS[array])
    return 1, start + plane - (REACH + extent_x)


def vmem_array(shape):
    return pltpu.VMEM(shape, jnp.float32)


def vmem_result(shape):
    return vmem_array(shape)


def in_vmem(array):
    return pltpu.with_memory_space_constraint(array, pltpu.VMEM)


vmem = pl.BlockSpec(memory_space=pltpu.VMEM)
leave = pl.BlockSpec(memory_space=pl.ANY)
limits = pltpu.CompilerParams(vmem_limit_bytes=24 * 2**20)


def strip_length(extent_x):
    own = extent_x * len(own_rows())
    return own, own + sum(rows for _, _, rows in corner_rows(extent_x))


def pack_own(arrays):
    extent_x, extent_y = arrays[0].shape[:2]
    last = extent_y // TILE - 1
    length = strip_length(extent_x)[0]

    def kernel(*refs):
        low_refs, high_refs, up_ref, down_ref = refs[0:3], refs[3:6], refs[6], refs[7]
        for k, (array, row) in enumerate(own_rows()):
            rows = slice(k * extent_x, (k + 1) * extent_x)
            up_ref[rows, :] = high_refs[array][:, TILE - WIDTHS[array] + row, :]
            down_ref[rows, :] = low_refs[array][:, row, :]

    def edge(array, block):
        return pl.BlockSpec((array.shape[0], TILE, LANES), lambda i: (0, block, 0))

    return pl.pallas_call(
        kernel,
        grid=(1,),
        in_specs=[edge(a, 0) for a in arrays] + [edge(a, last) for a in arrays],
        out_specs=[vmem] * 2,
        out_shape=[vmem_result((length, LANES))] * 2,
        compiler_params=limits,
        name="pack_own",
    )(*arrays, *arrays)


def pack_corners(strips, slabs, extent_x):
    own, length = strip_length(extent_x)

    def kernel(own_up, own_down, low_ref, high_ref, up_ref, down_ref):
        up_ref[0:own, :] = own_up[...]
        down_ref[0:own, :] = own_down[...]
        at = own
        for array, plane, rows in corner_rows(extent_x):
            side, where = slab_plane(array, plane, extent_x)
            slab = (low_ref, high_ref)[side]
            last = slab.shape[1]
            up_ref[at : at + rows, :] = slab[where, last - rows : last, :]
            down_ref[at : at + rows, :] = slab[where, 0:rows, :]
            at += rows

    return pl.pallas_call(
        kernel,
        in_specs=[vmem] * 4,
        out_specs=[vmem] * 2,
        out_shape=[vmem_result((length, LANES))] * 2,
        compiler_params=limits,
        name="pack_corners",
    )(*map(in_vmem, strips), *map(in_vmem, slabs))


def plane_rolls(values, axis):
    return pltpu.roll(values, values.shape[axis] - 1, axis), pltpu.roll(values, 1, axis)


def coefficients(cond, cond_next, face_west):
    lane = lax.broadcasted_iota(jnp.int32, cond.shape, 1)
    cond_up, cond_down = plane_rolls(cond, 1)
    face_east = 0.5 * (cond + cond_next)
    face_north = 0.5 * (cond + plane_rolls(cond, 0)[0])
    face_south = plane_rolls(face_north, 0)[1]
    face_up = jnp.where(lane < LANES - 1, 0.5 * (cond + cond_up), 0.0)
    face_down = jnp.where(lane > 0, 0.5 * (cond + cond_down), 0.0)
    diagonal = (face_east + face_west) + (face_north + face_south) + (face_up + face_down)
    scale = jnp.where(cond > 0, relax_weight / diagonal, 0.0)
    return face_east, face_north, face_south, face_up, face_down, scale


def prepare(first, size, cond_ref, face_refs, face_west):
    limit = cond_ref.shape[0] - 1
    for k in range(size):
        plane = first + k
        made = coefficients(cond_ref[plane], cond_ref[jnp.minimum(plane + 1, limit)], face_west)
        for ref, part in zip(face_refs, made):
            ref[plane] = part
        face_west = made[0]
    return face_west


def sweep(low, count, size, value_ref, source_ref, face_refs, term_ref, store):
    face_x, face_n, face_s, face_u, face_d, scales = face_refs
    limit = value_ref.shape[0] - 1

    def make_terms(planes, rolled):
        for plane, (up, down) in zip(planes, rolled):
            term_ref[plane] = face_u[plane] * up + face_d[plane] * down

    def block(index, carried):
        before, value, face_west = carried
        base = low + index * size
        ahead = [jnp.minimum(base + size + k, limit) for k in range(size)]
        rolled = [plane_rolls(value_ref[plane], 1) for plane in ahead]
        for k in range(size):
            plane = base + k
            value_next = value_ref[plane + 1]
            face_east = face_x[plane]
            north, south = plane_rolls(value, 0)
            near = (face_east * value_next + face_west * before) + (
                face_n[plane] * north + face_s[plane] * south
            )
            near = (near + term_ref[plane]) + source_ref[plane]
            store(index, k, plane, (1.0 - relax_weight) * value + scales[plane] * near)
            before, value, face_west = value, value_next, face_east
        make_terms(ahead, rolled)
        return before, value, face_west

    planes = [low + k for k in range(size)]
    make_terms(planes, [plane_rolls(value_ref[plane], 1) for plane in planes])
    start = (value_ref[low - 1], value_ref[low], face_x[low - 1])
    lax.fori_loop(0, count // size, block, start)


def keep_in(ref):
    def store(index, k, plane, value):
        ref[plane] = value

    return store


def start_copies(pairs, sems):
    copies = [pltpu.make_async_copy(a, b, sems.at[k]) for k, (a, b) in enumerate(pairs)]
    for copy in copies:
        copy.start()
    return copies


def own_part(ext, extent_x, extent_y):
    return ext.at[pl.ds(REACH, extent_x), pl.ds(TILE, extent_y)]


def place_halos(ext_refs, slab_refs, strip_refs, extent_x, extent_y, arrays):
    inner = slice(TILE, TILE + extent_y)
    for array in arrays:
        ext, width = ext_refs[array], WIDTHS[array]
        planes = ext.shape[0]
        zeros = jnp.zeros((planes, TILE, LANES), jnp.float32)
        ext[:, 0:TILE, :] = zeros
        ext[:, TILE + extent_y : 2 * TILE + extent_y, :] = zeros
        for plane in range(REACH - width):
            for side in (plane, planes - 1 - plane):
                ext[side, inner, :] = jnp.zeros((extent_y, LANES), jnp.float32)
        start = sum(WIDTHS[:array])
        part = slice(start, start + width)
        ext[REACH - width : REACH, inner, :] = slab_refs[0][part]
        ext[REACH + extent_x : REACH + extent_x + width, inner, :] = slab_refs[1][part]
    low_ref, high_ref = strip_refs
    for k, (array, row) in enumerate(own_rows()):
        if array in arrays:
            ext, rows = ext_refs[array], slice(k * extent_x, (k + 1) * extent_x)
            own = slice(REACH, REACH + extent_x)
            ext[own, TILE - WIDTHS[array] + row, :] = low_ref[rows, :]
            ext[own, TILE + extent_y + row, :] = high_ref[rows, :]
    at = strip_length(extent_x)[0]
    for array, plane, rows in corner_rows(extent_x):
        if array in arrays:
            ext = ext_refs[array]
            ext[plane, TILE - rows : TILE, :] = low_ref[at : at + rows, :]
            ext[plane, TILE + extent_y : TILE + extent_y + rows, :] = high_ref[at : at + rows, :]
        at += rows


def before_kernel(
    cond_in, source_in, value_in, slab_low, slab_high, strip_low, strip_high, row_ref, value_out,
    cond_ext, source_ext, value_ext, other, term, face_x, face_n, face_s, face_u, face_d, scales,
    sems, out_sem,
):
    extent_x, extent_y = cond_in.shape[0], cond_in.shape[1]
    planes = extent_x + 2 * REACH
    exts = (cond_ext, source_ext, value_ext)
    face_refs = (face_x, face_n, face_s, face_u, face_d, scales)
    pairs = [
        (ref, own_part(ext, extent_x, extent_y))
        for ref, ext in zip((cond_in, source_in, value_in), exts)
    ]
    copies = start_copies(pairs, sems)
    place_halos(
        exts, (slab_low, slab_high), (strip_low, strip_high), extent_x, extent_y, (0, 1, 2)
    )
    blank = jnp.zeros(cond_ext.shape[1:], jnp.float32)
    other[0] = blank
    other[planes - 1] = blank
    for copy in copies:
        copy.wait()

    def prepare_block(index, face_west):
        return prepare(4 * index, 4, cond_ext, face_refs, face_west)

    lax.fori_loop(0, planes // 4, prepare_block, blank)
    shared = (source_ext, face_refs, term)
    sweep(1, planes - 2, 3, value_ext, *shared, keep_in(other))
    sweep(1, planes - 2, 3, other, *shared, keep_in(value_ext))
    sweep(1, planes - 2, 3, value_ext, *shared, keep_in(other))
    kept = pltpu.make_async_copy(other.at[pl.ds(NU, planes - 2 * NU)], value_out, out_sem)
    kept.start()

    inner = slice(TILE, TILE + extent_y)
    low_x, high_x = REACH, REACH + extent_x - 1
    east = face_x[high_x, inner, :]
    west = face_x[low_x - 1, inner, :]
    net = east * (other[high_x + 1, inner, :] - other[high_x, inner, :]) + west * (
        other[low_x - 1, inner, :] - other[low_x, inner, :]
    )
    edge_low, edge_high = slice(0, 2 * TILE), slice(extent_y, extent_y + 2 * TILE)
    zero = jnp.zeros((extent_y, LANES), jnp.float32)
    zero_edge = jnp.zeros((2 * TILE, LANES), jnp.float32)

    def along(index, carried):
        sources, flow_low, flow_high, face_low, face_high = carried
        for k in range(4):
            plane = low_x + 4 * index + k
            sources = sources + source_ext[plane, inner, :]
            value = other[plane, edge_low, :]
            face = face_n[plane, edge_low, :]
            flow_low = flow_low + face * (plane_rolls(value, 0)[0] - value)
            face_low = face_low + face
            value = other[plane, edge_high, :]
            face = face_n[plane, edge_high, :]
            flow_high = flow_high + face * (plane_rolls(value, 0)[0] - value)
            face_high = face_high + face
        return sources, flow_low, flow_high, face_low, face_high

    sources, flow_low, flow_high, face_low, face_high = lax.fori_loop(
        0, extent_x // 4, along, (zero, zero_edge, zero_edge, zero_edge, zero_edge)
    )
    edge_row = lax.broadcasted_iota(jnp.int32, zero_edge.shape, 0) == TILE - 1

    def whole(values):
        return jnp.sum(jnp.sum(values, axis=0, keepdims=True), axis=1, keepdims=True)

    def face_sum(values):
        return whole(jnp.where(edge_row, values, 0.0))

    flow_north, flow_south = face_sum(face_high), face_sum(face_low)
    flow_east, flow_west = whole(east), whole(west)
    residual = whole(sources + net) + (face_sum(flow_high) - face_sum(flow_low))
    diag = flow_east + flow_west + flow_north + flow_south
    place = lax.broadcasted_iota(jnp.int32, row_ref.shape, 1) - lax.axis_index("gy")
    row = jnp.where(place == 3 * SIDE, flow_north, 0.0)
    row = jnp.where(place == 2 * SIDE, flow_east, row)
    row = jnp.where(place == SIDE, diag, row)
    row_ref[...] = jnp.where(place == 0, residual, row)
    kept.wait()


def total(values):
    return jnp.sum(jnp.sum(values, axis=1, keepdims=True), axis=0, keepdims=True)


def brick_index(shape):
    sublane = lax.broadcasted_iota(jnp.int32, shape, 0)
    lane = lax.broadcasted_iota(jnp.int32, shape, 1)
    return lane // SIDE * TILE + sublane, lane % SIDE


def fold(packed_ref, turn, part):
    lane = lax.broadcasted_iota(jnp.int32, (TILE, LANES), 1)
    folded = jnp.zeros((TILE, LANES), jnp.float32)
    for group in range(LANES // SIDE):
        start = (group + turn) % (SIDE // TILE) * TILE
        rows = packed_ref[start : start + TILE, :]
        shift = SIDE * (group - part) % LANES
        rows = pltpu.roll(rows, shift, 1) if shift else rows
        folded = jnp.where(lane // SIDE == group, rows, folded)
    return folded


def around(values):
    sublane = lax.broadcasted_iota(jnp.int32, values.shape, 0)
    ahead, behind = plane_rolls(values, 0)
    return (
        jnp.where(sublane == TILE - 1, pltpu.roll(ahead, LANES - SIDE, 1), ahead),
        jnp.where(sublane == 0, pltpu.roll(behind, SIDE, 1), behind),
        pltpu.roll(values, LANES - 1, 1),
        pltpu.roll(values, 1, 1),
    )


def coarse_solver(packed_ref, turn, count_x, count_y):
    start, diag, east, north = (fold(packed_ref, turn, part) for part in range(4))
    brick_x, brick_y = brick_index(start.shape)
    east = jnp.where(brick_x < count_x - 1, east, 0.0)
    north = jnp.where(brick_y < count_y - 1, north, 0.0)
    west, south = around(east)[1], around(north)[3]

    def products(remainder, beside):
        image = (
            diag * remainder
            - (east * beside[0] + west * beside[1])
            - (north * beside[2] + south * beside[3])
        )
        return image, around(image), total(remainder * remainder), total(image * remainder)

    def moved(state, alpha, norm, search, image, image_beside):
        estimate, remainder, beside = state
        estimate = estimate + alpha * search
        remainder = remainder - alpha * image
        beside = tuple(b - alpha * i for b, i in zip(beside, image_beside))
        return estimate, remainder, beside, search, image, image_beside, norm, alpha

    beside = around(start)
    image, image_beside, norm, curve = products(start, beside)
    first = moved(
        (jnp.zeros_like(start), start, beside), norm / curve, norm, start, image, image_beside
    )

    def iterate_once(carried):
        estimate, remainder, beside, search, image, image_beside, norm_before, alpha = carried
        new_image, new_beside, norm, curve = products(remainder, beside)
        beta = norm / norm_before
        alpha = norm / (curve - beta * norm / alpha)
        search = remainder + beta * search
        image = new_image + beta * image
        image_beside = tuple(n + beta * i for n, i in zip(new_beside, image_beside))
        return moved(
            (estimate, remainder, beside), alpha, norm, search, image, image_beside
        )

    return first, iterate_once


def after_kernel(turn, counts):
    def kernel(
        packed_ref, cond_in, source_in, value_in, slab_low, slab_high, strip_low, strip_high,
        out_ref, cond_ext, source_ext, value_ext, other, term, face_x, face_n, face_s, face_u,
        face_d, scales, out_part, sems, out_sems,
    ):
        extent_x, extent_y = cond_in.shape[0], cond_in.shape[1]
        planes = extent_x + 2 * REACH
        exts = (cond_ext, source_ext)
        face_refs = (face_x, face_n, face_s, face_u, face_d, scales)
        copies = start_copies(
            [
                (cond_in, own_part(cond_ext, extent_x, extent_y)),
                (source_in, own_part(source_ext, extent_x, extent_y)),
                (value_in, value_ext.at[pl.ds(NU, planes - 2 * NU)]),
            ],
            sems,
        )
        place_halos(
            exts, (slab_low, slab_high), (strip_low, strip_high), extent_x, extent_y, (0, 1)
        )
        state, iterate_once = coarse_solver(packed_ref, turn, *counts)
        low = NU + 1
        pairs = (planes - 2 * low) // 2
        lead = min(6, max(CG_ITERS - 1 - pairs, 0))
        state = lax.fori_loop(0, lead, lambda i, s: iterate_once(s), state)
        for copy in copies:
            copy.wait()
        face_west = 0.5 * (cond_ext[low - 1] + cond_ext[low])
        face_x[low - 1] = face_west

        def both(index, carried):
            face_west = prepare(low + 2 * index, 2, cond_ext, face_refs, carried[1])
            return iterate_once(carried[0]), face_west

        shared = min(pairs, CG_ITERS - 1 - lead)
        state, face_west = lax.fori_loop(0, shared, both, (state, face_west))
        if shared < pairs:
            prepare(low + 2 * shared, 2 * (pairs - shared), cond_ext, face_refs, face_west)
        rest = CG_ITERS - 1 - lead - shared
        state = lax.fori_loop(0, rest, lambda i, s: iterate_once(s), state)
        estimate = state[0]

        brick_x, brick_y = brick_index(estimate.shape)
        step_x = brick_x - lax.axis_index("gx")
        step_y = brick_y - lax.axis_index("gy")
        row = lax.broadcasted_iota(jnp.int32, cond_ext.shape[1:], 0)

        def lift_of(step):
            low, own, high = (
                total(jnp.where((step_x == step) & (step_y == side), estimate, 0.0))
                for side in (-1, 0, 1)
            )
            return jnp.where(row < TILE, low, jnp.where(row < TILE + extent_y, own, high))

        lifts = [lift_of(step) for step in (-1, 0, 1)]

        def lift(plane, amount):
            inside = cond_ext[plane] > 0
            value_ext[plane] = value_ext[plane] + jnp.where(inside, amount, 0.0)

        for k in range(NU):
            lift(NU + k, lifts[0])
            lift(REACH + extent_x + k, lifts[2])

        def lift_block(index, carried):
            for k in range(4):
                lift(REACH + 4 * index + k, lifts[1])
            return carried

        lax.fori_loop(0, extent_x // 4, lift_block, 0)

        shared = (source_ext, face_refs, term)
        sweep(low, planes - 2 * low, 3, value_ext, *shared, keep_in(other))
        sweep(low + 1, planes - 2 * low, 3, other, *shared, keep_in(value_ext))
        size = 4

        def part(index):
            rows = pl.ds(index * size, size)
            return pltpu.make_async_copy(out_part.at[rows], out_ref.at[rows], out_sems.at[index])

        def finish(index, k, plane, value):
            out_part[index * size + k] = value[TILE : TILE + extent_y]
            if k == size - 1:
                part(index).start()

        sweep(REACH, extent_x, size, value_ext, *shared, finish)
        for index in range(extent_x // size):
            part(index).wait()

    return kernel


def spread(rows, axis, order):
    return lax.all_to_all(rows, axis, 0, 0, tiled=True, axis_index_groups=[order])


def body(conductivity, source, initial):
    arrays = (conductivity, source, initial)
    extent_x, extent_y = conductivity.shape[:2]
    count_x, count_y = lax.axis_size("gx"), lax.axis_size("gy")
    tails = jnp.concatenate([a[extent_x - w :] for a, w in zip(arrays, WIDTHS)], 0)
    heads = jnp.concatenate([a[:w] for a, w in zip(arrays, WIDTHS)], 0)
    slabs = (
        lax.ppermute(tails, "gx", ring_pairs(count_x, 1)),
        lax.ppermute(heads, "gx", ring_pairs(count_x, -1)),
    )
    up, down = pack_corners(pack_own(arrays), slabs, extent_x)
    strips = (
        lax.ppermute(up, "gy", ring_pairs(count_y, 1)),
        lax.ppermute(down, "gy", ring_pairs(count_y, -1)),
    )
    halos = [in_vmem(a) for a in (*slabs, *strips)]
    planes, rows = extent_x + 2 * REACH, extent_y + 2 * TILE
    scratch = [vmem_array((planes, rows, LANES))] * 11 + [pltpu.SemaphoreType.DMA((3,))]
    row, smoothed = pl.pallas_call(
        before_kernel,
        in_specs=[leave] * 3 + [vmem] * 4,
        out_specs=[vmem, leave],
        out_shape=[
            jax.ShapeDtypeStruct((count_y, LANES), jnp.float32),
            jax.ShapeDtypeStruct((planes - 2 * NU, rows, LANES), jnp.float32),
        ],
        scratch_shapes=scratch + [pltpu.SemaphoreType.DMA],
        compiler_params=limits,
        name="smooth_before",
    )(*arrays, *halos)
    row = jnp.sum(spread(row, "gy", list(range(count_y))), axis=0, keepdims=True)
    half = count_x // 2
    order = list(range(half, count_x)) + list(range(half))
    packed = spread(jnp.broadcast_to(row, (count_x, LANES)), "gx", order)
    turn = SIDE // TILE // 2
    if count_x != SIDE:
        packed = jnp.pad(jnp.roll(packed, half, 0), ((0, SIDE - count_x), (0, 0)))
        turn = 0
    return pl.pallas_call(
        after_kernel(turn, (count_x, count_y)),
        in_specs=[vmem] + [leave] * 3 + [vmem] * 4,
        out_specs=leave,
        out_shape=jax.ShapeDtypeStruct(conductivity.shape, jnp.float32),
        scratch_shapes=scratch[:-1]
        + [vmem_array(conductivity.shape), scratch[-1], pltpu.SemaphoreType.DMA((extent_x // 4,))],
        compiler_params=limits,
        name="smooth_after",
    )(packed, conductivity, source, smoothed, *halos)


def solution(mesh):
    return jax.shard_map(
        body,
        mesh=mesh,
        in_specs=(P("gx", "gy", None), P("gx", "gy", None), P("gx", "gy", None)),
        out_specs=P("gx", "gy", None),
        check_vma=False,
    )
```

```python
import jax
import jax.numpy as jnp
from jax import lax
from jax.experimental import pallas as pl
from jax.experimental.pallas import tpu as pltpu
from jax.sharding import PartitionSpec as P

NU = 3
CG_ITERS = 32


relax_weight = 0.8
REACH = 2 * NU
WIDTHS = (REACH, REACH - 1, REACH)
LANES = 128
TILE = 8
SIDE = 32


def ring_pairs(count, step):
    return [(i, i + step) for i in range(count) if 0 <= i + step < count]


def own_rows():
    return [(array, row) for array, width in enumerate(WIDTHS) for row in range(width)]


def corner_rows(extent_x):
    rows = []
    for array, width in enumerate(WIDTHS):
        for beyond in range(1, width):
            for plane in (REACH - beyond, REACH + extent_x - 1 + beyond):
                rows.append((array, plane, width - beyond))
    return rows


def slab_plane(array, plane, extent_x):
    start = sum(WIDTHS[:array])
    if plane < REACH:
        return 0, start + plane - (REACH - WIDTHS[array])
    return 1, start + plane - (REACH + extent_x)


def vmem_array(shape):
    return pltpu.VMEM(shape, jnp.float32)


def vmem_result(shape):
    return vmem_array(shape)


def in_vmem(array):
    return pltpu.with_memory_space_constraint(array, pltpu.VMEM)


def in_hbm(array):
    return pltpu.with_memory_space_constraint(array, pltpu.HBM)


vmem = pl.BlockSpec(memory_space=pltpu.VMEM)
leave = pl.BlockSpec(memory_space=pl.ANY)
limits = pltpu.CompilerParams(vmem_limit_bytes=24 * 2**20)


def pack_slabs(arrays):
    extent_x = arrays[0].shape[0]
    shape = (sum(WIDTHS), *arrays[0].shape[1:])

    def kernel(*refs):
        tails, heads, sems = refs[3:]
        copies = []
        for ref, width, at in zip(refs[:3], WIDTHS, (0, WIDTHS[0], WIDTHS[0] + WIDTHS[1])):
            for start, target in ((extent_x - width, tails), (0, heads)):
                source = ref.at[pl.ds(start, width)]
                sem = sems.at[len(copies)]
                copies.append(pltpu.make_async_copy(source, target.at[pl.ds(at, width)], sem))
        for copy in copies:
            copy.start()
        for copy in copies:
            copy.wait()

    return pl.pallas_call(
        kernel,
        in_specs=[pl.BlockSpec(memory_space=pltpu.HBM)] * 3,
        out_specs=[vmem] * 2,
        out_shape=[vmem_result(shape)] * 2,
        scratch_shapes=[pltpu.SemaphoreType.DMA((6,))],
        compiler_params=limits,
        name="pack_slabs",
    )(*map(in_hbm, arrays))


def pack_own(arrays):
    extent_x, extent_y = arrays[0].shape[:2]
    last = extent_y // TILE - 1
    length = extent_x * len(own_rows())

    def kernel(*refs):
        low_refs, high_refs, up_ref, down_ref = refs[0:3], refs[3:6], refs[6], refs[7]
        for k, (array, row) in enumerate(own_rows()):
            rows = slice(k * extent_x, (k + 1) * extent_x)
            up_ref[rows, :] = high_refs[array][:, TILE - WIDTHS[array] + row, :]
            down_ref[rows, :] = low_refs[array][:, row, :]

    def edge(array, block):
        return pl.BlockSpec((array.shape[0], TILE, LANES), lambda i: (0, block, 0))

    return pl.pallas_call(
        kernel,
        grid=(1,),
        in_specs=[edge(a, 0) for a in arrays] + [edge(a, last) for a in arrays],
        out_specs=[vmem] * 2,
        out_shape=[vmem_result((length, LANES))] * 2,
        compiler_params=limits,
        name="pack_own",
    )(*arrays, *arrays)


def pack_corners(slabs, extent_x):
    length = sum(rows for _, _, rows in corner_rows(extent_x))

    def kernel(low_ref, high_ref, up_ref, down_ref):
        at = 0
        for array, plane, rows in corner_rows(extent_x):
            side, where = slab_plane(array, plane, extent_x)
            slab = (low_ref, high_ref)[side]
            last = slab.shape[1]
            up_ref[at : at + rows, :] = slab[where, last - rows : last, :]
            down_ref[at : at + rows, :] = slab[where, 0:rows, :]
            at += rows

    return pl.pallas_call(
        kernel,
        in_specs=[vmem] * 2,
        out_specs=[vmem] * 2,
        out_shape=[vmem_result((length, LANES))] * 2,
        compiler_params=limits,
        name="pack_corners",
    )(*map(in_vmem, slabs))


def plane_rolls(values, axis):
    return pltpu.roll(values, values.shape[axis] - 1, axis), pltpu.roll(values, 1, axis)


def coefficients(cond, cond_next, face_west):
    lane = lax.broadcasted_iota(jnp.int32, cond.shape, 1)
    cond_up, cond_down = plane_rolls(cond, 1)
    face_east = 0.5 * (cond + cond_next)
    face_north = 0.5 * (cond + plane_rolls(cond, 0)[0])
    face_south = plane_rolls(face_north, 0)[1]
    face_up = jnp.where(lane < LANES - 1, 0.5 * (cond + cond_up), 0.0)
    face_down = jnp.where(lane > 0, 0.5 * (cond + cond_down), 0.0)
    diagonal = (face_east + face_west) + (face_north + face_south) + (face_up + face_down)
    scale = jnp.where(cond > 0, relax_weight / diagonal, 0.0)
    return face_east, face_north, face_south, face_up, face_down, scale


def prepare(first, size, cond_ref, face_refs, face_west):
    limit = cond_ref.shape[0] - 1
    for k in range(size):
        plane = first + k
        made = coefficients(cond_ref[plane], cond_ref[jnp.minimum(plane + 1, limit)], face_west)
        for ref, part in zip(face_refs, made):
            ref[plane] = part
        face_west = made[0]
    return face_west


def sweep(low, count, size, value_ref, source_ref, face_refs, term_ref, store, rows=slice(None)):
    face_x, face_n, face_s, face_u, face_d, scales = face_refs
    limit = value_ref.shape[0] - 1

    def make_terms(planes, rolled):
        for plane, (up, down) in zip(planes, rolled):
            term_ref[plane, rows] = face_u[plane, rows] * up[rows] + face_d[plane, rows] * down[rows]

    def block(index, carried):
        before, value, face_west = carried
        base = low + index * size
        ahead = [jnp.minimum(base + size + k, limit) for k in range(size)]
        rolled = [plane_rolls(value_ref[plane], 1) for plane in ahead]
        for k in range(size):
            plane = base + k
            value_next = value_ref[plane + 1]
            face_east = face_x[plane, rows]
            north, south = plane_rolls(value, 0)
            near = (face_east * value_next[rows] + face_west * before) + (
                face_n[plane, rows] * north[rows] + face_s[plane, rows] * south[rows]
            )
            near = (near + term_ref[plane, rows]) + source_ref[plane, rows]
            value_own = value[rows]
            store(index, k, plane, (1.0 - relax_weight) * value_own + scales[plane, rows] * near)
            before, value, face_west = value_own, value_next, face_east
        make_terms(ahead, rolled)
        return before, value, face_west

    planes = [low + k for k in range(size)]
    make_terms(planes, [plane_rolls(value_ref[plane], 1) for plane in planes])
    start = (value_ref[low - 1, rows], value_ref[low], face_x[low - 1, rows])
    lax.fori_loop(0, count // size, block, start)


def keep_in(ref):
    def store(index, k, plane, value):
        ref[plane] = value

    return store


def start_copies(pairs, sems):
    copies = [pltpu.make_async_copy(a, b, sems.at[k]) for k, (a, b) in enumerate(pairs)]
    for copy in copies:
        copy.start()
    return copies


def own_part(ext, extent_x, extent_y):
    return ext.at[pl.ds(REACH, extent_x), pl.ds(TILE, extent_y)]


def place_halos(ext_refs, slab_refs, strip_refs, corner_refs, extent_x, extent_y):
    inner = slice(TILE, TILE + extent_y)
    for ext, width, start in zip(ext_refs, WIDTHS, (0, WIDTHS[0], WIDTHS[0] + WIDTHS[1])):
        planes = ext.shape[0]
        zeros = jnp.zeros((planes, TILE, LANES), jnp.float32)
        ext[:, 0:TILE, :] = zeros
        ext[:, TILE + extent_y : 2 * TILE + extent_y, :] = zeros
        for plane in range(REACH - width):
            for side in (plane, planes - 1 - plane):
                ext[side, inner, :] = jnp.zeros((extent_y, LANES), jnp.float32)
        part = slice(start, start + width)
        ext[REACH - width : REACH, inner, :] = slab_refs[0][part]
        ext[REACH + extent_x : REACH + extent_x + width, inner, :] = slab_refs[1][part]
    for k, (array, row) in enumerate(own_rows()):
        ext, rows = ext_refs[array], slice(k * extent_x, (k + 1) * extent_x)
        own = slice(REACH, REACH + extent_x)
        ext[own, TILE - WIDTHS[array] + row, :] = strip_refs[0][rows, :]
        ext[own, TILE + extent_y + row, :] = strip_refs[1][rows, :]
    at = 0
    for array, plane, rows in corner_rows(extent_x):
        ext, part = ext_refs[array], slice(at, at + rows)
        ext[plane, TILE - rows : TILE, :] = corner_refs[0][part, :]
        ext[plane, TILE + extent_y : TILE + extent_y + rows, :] = corner_refs[1][part, :]
        at += rows


def before_kernel(
    cond_in, source_in, value_in, slab_low, slab_high, strip_low, strip_high, corner_low,
    corner_high, row_ref, other, source_ext, face_x, face_n, face_s, face_u, face_d, scales,
    cond_ext, value_ext, term, sems,
):
    extent_x, extent_y = cond_in.shape[0], cond_in.shape[1]
    planes = extent_x + 2 * REACH
    exts = (cond_ext, source_ext, value_ext)
    face_refs = (face_x, face_n, face_s, face_u, face_d, scales)
    pairs = [
        (ref, own_part(ext, extent_x, extent_y))
        for ref, ext in zip((cond_in, source_in, value_in), exts)
    ]
    copies = start_copies(pairs, sems)
    place_halos(
        exts,
        (slab_low, slab_high),
        (strip_low, strip_high),
        (corner_low, corner_high),
        extent_x,
        extent_y,
    )
    blank = jnp.zeros(cond_ext.shape[1:], jnp.float32)
    other[0] = blank
    other[planes - 1] = blank
    for copy in copies:
        copy.wait()

    def prepare_block(index, face_west):
        return prepare(11 * index, 11, cond_ext, face_refs, face_west)

    lax.fori_loop(0, planes // 11, prepare_block, blank)
    shared = (source_ext, face_refs, term)
    sweep(1, planes - 2, 14, value_ext, *shared, keep_in(other))
    sweep(1, planes - 2, 14, other, *shared, keep_in(value_ext))
    sweep(1, planes - 2, 14, value_ext, *shared, keep_in(other))

    inner = slice(TILE, TILE + extent_y)
    low_x, high_x = REACH, REACH + extent_x - 1
    east = face_x[high_x, inner, :]
    west = face_x[low_x - 1, inner, :]
    net = east * (other[high_x + 1, inner, :] - other[high_x, inner, :]) + west * (
        other[low_x - 1, inner, :] - other[low_x, inner, :]
    )
    edge_low, edge_high = slice(0, 2 * TILE), slice(extent_y, extent_y + 2 * TILE)
    zero = jnp.zeros((extent_y, LANES), jnp.float32)
    zero_edge = jnp.zeros((2 * TILE, LANES), jnp.float32)

    def along(index, carried):
        sources, flow_low, flow_high, face_low, face_high = carried
        for k in range(4):
            plane = low_x + 4 * index + k
            sources = sources + source_ext[plane, inner, :]
            value = other[plane, edge_low, :]
            face = face_n[plane, edge_low, :]
            flow_low = flow_low + face * (plane_rolls(value, 0)[0] - value)
            face_low = face_low + face
            value = other[plane, edge_high, :]
            face = face_n[plane, edge_high, :]
            flow_high = flow_high + face * (plane_rolls(value, 0)[0] - value)
            face_high = face_high + face
        return sources, flow_low, flow_high, face_low, face_high

    sources, flow_low, flow_high, face_low, face_high = lax.fori_loop(
        0, extent_x // 4, along, (zero, zero_edge, zero_edge, zero_edge, zero_edge)
    )
    edge_row = lax.broadcasted_iota(jnp.int32, zero_edge.shape, 0) == TILE - 1

    def whole(values):
        return jnp.sum(jnp.sum(values, axis=0, keepdims=True), axis=1, keepdims=True)

    def face_sum(values):
        return whole(jnp.where(edge_row, values, 0.0))

    flow_north, flow_south = face_sum(face_high), face_sum(face_low)
    flow_east, flow_west = whole(east), whole(west)
    residual = whole(sources + net) + (face_sum(flow_high) - face_sum(flow_low))
    diag = flow_east + flow_west + flow_north + flow_south
    place = lax.broadcasted_iota(jnp.int32, row_ref.shape, 1) - lax.axis_index("gy")
    row = jnp.where(place == 3 * SIDE, flow_north, 0.0)
    row = jnp.where(place == 2 * SIDE, flow_east, row)
    row = jnp.where(place == SIDE, diag, row)
    row_ref[...] = jnp.where(place == 0, residual, row)


def total(values):
    return jnp.sum(jnp.sum(values, axis=1, keepdims=True), axis=0, keepdims=True)


def brick_index(shape):
    sublane = lax.broadcasted_iota(jnp.int32, shape, 0)
    lane = lax.broadcasted_iota(jnp.int32, shape, 1)
    return lane // SIDE * TILE + sublane, lane % SIDE


def fold(packed_ref, turn, part):
    lane = lax.broadcasted_iota(jnp.int32, (TILE, LANES), 1)
    folded = jnp.zeros((TILE, LANES), jnp.float32)
    for group in range(LANES // SIDE):
        start = (group + turn) % (SIDE // TILE) * TILE
        rows = packed_ref[start : start + TILE, :]
        shift = SIDE * (group - part) % LANES
        rows = pltpu.roll(rows, shift, 1) if shift else rows
        folded = jnp.where(lane // SIDE == group, rows, folded)
    return folded


def around(values):
    sublane = lax.broadcasted_iota(jnp.int32, values.shape, 0)
    ahead, behind = plane_rolls(values, 0)
    return (
        jnp.where(sublane == TILE - 1, pltpu.roll(ahead, LANES - SIDE, 1), ahead),
        jnp.where(sublane == 0, pltpu.roll(behind, SIDE, 1), behind),
        pltpu.roll(values, LANES - 1, 1),
        pltpu.roll(values, 1, 1),
    )


def coarse_solver(packed_ref, turn, count_x, count_y):
    start, diag, east, north = (fold(packed_ref, turn, part) for part in range(4))
    brick_x, brick_y = brick_index(start.shape)
    east = jnp.where(brick_x < count_x - 1, east, 0.0)
    north = jnp.where(brick_y < count_y - 1, north, 0.0)
    west, south = around(east)[1], around(north)[3]

    def products(remainder, beside):
        image = (
            diag * remainder
            - (east * beside[0] + west * beside[1])
            - (north * beside[2] + south * beside[3])
        )
        return image, around(image), total(remainder * remainder), total(image * remainder)

    def moved(state, alpha, norm, search, image, image_beside):
        estimate, remainder, beside = state
        estimate = estimate + alpha * search
        remainder = remainder - alpha * image
        beside = tuple(b - alpha * i for b, i in zip(beside, image_beside))
        return estimate, remainder, beside, search, image, image_beside, norm, alpha

    beside = around(start)
    image, image_beside, norm, curve = products(start, beside)
    first = moved(
        (jnp.zeros_like(start), start, beside), norm / curve, norm, start, image, image_beside
    )

    def iterate_once(carried):
        estimate, remainder, beside, search, image, image_beside, norm_before, alpha = carried
        new_image, new_beside, norm, curve = products(remainder, beside)
        beta = norm / norm_before
        alpha = norm / (curve - beta * norm / alpha)
        search = remainder + beta * search
        image = new_image + beta * image
        image_beside = tuple(n + beta * i for n, i in zip(new_beside, image_beside))
        return moved(
            (estimate, remainder, beside), alpha, norm, search, image, image_beside
        )

    return first, iterate_once


def after_kernel(turn, counts):
    def kernel(
        packed_ref, value_in, source_ext, face_x, face_n, face_s, face_u, face_d, scales, out_ref,
        value_ext, other, term, out_part, out_sems,
    ):
        extent_x, extent_y = out_ref.shape[0], out_ref.shape[1]
        planes = extent_x + 2 * REACH
        face_refs = (face_x, face_n, face_s, face_u, face_d, scales)
        low = NU + 1
        state, iterate_once = coarse_solver(packed_ref, turn, *counts)
        state = lax.fori_loop(0, CG_ITERS - 1, lambda i, s: iterate_once(s), state)
        estimate = state[0]

        brick_x, brick_y = brick_index(estimate.shape)
        step_x = brick_x - lax.axis_index("gx")
        step_y = brick_y - lax.axis_index("gy")
        row = lax.broadcasted_iota(jnp.int32, value_in.shape[1:], 0)

        def lift_of(step):
            low, own, high = (
                total(jnp.where((step_x == step) & (step_y == side), estimate, 0.0))
                for side in (-1, 0, 1)
            )
            return jnp.where(row < TILE, low, jnp.where(row < TILE + extent_y, own, high))

        lifts = [lift_of(step) for step in (-1, 0, 1)]

        def lift(plane, amount):
            inside = scales[plane] > 0
            value_ext[plane] = value_in[plane] + jnp.where(inside, amount, 0.0)

        for k in range(NU):
            lift(NU + k, lifts[0])
            lift(REACH + extent_x + k, lifts[2])

        def lift_block(index, carried):
            for k in range(4):
                lift(REACH + 4 * index + k, lifts[1])
            return carried

        lax.fori_loop(0, extent_x // 4, lift_block, 0)

        shared = (source_ext, face_refs, term)
        sweep(low, planes - 2 * low, 12, value_ext, *shared, keep_in(other))
        sweep(low + 1, planes - 2 * low, 12, other, *shared, keep_in(value_ext))
        size = 8

        def part(index):
            rows = pl.ds(index * size, size)
            return pltpu.make_async_copy(out_part.at[rows], out_ref.at[rows], out_sems.at[index])

        def finish(index, k, plane, value):
            out_part[index * size + k] = value
            if k == size - 1:
                part(index).start()

        inner = slice(TILE, TILE + extent_y)
        sweep(REACH, extent_x, size, value_ext, *shared, finish, inner)
        for index in range(extent_x // size):
            part(index).wait()

    return kernel


def add_rows(gathered, count):
    def kernel(rows_ref, out_ref):
        row = jnp.sum(rows_ref[...], axis=0, keepdims=True)
        out_ref[...] = jnp.broadcast_to(row, out_ref.shape)

    return pl.pallas_call(
        kernel,
        in_specs=[vmem],
        out_specs=vmem,
        out_shape=vmem_result((count, LANES)),
        compiler_params=pltpu.CompilerParams(vmem_limit_bytes=2**20),
        name="add_rows",
    )(in_vmem(gathered))


def spread(rows, axis, order):
    return lax.all_to_all(rows, axis, 0, 0, tiled=True, axis_index_groups=[order])


def body(conductivity, source, initial):
    arrays = (conductivity, source, initial)
    extent_x, extent_y = conductivity.shape[:2]
    count_x, count_y = lax.axis_size("gx"), lax.axis_size("gy")
    tails, heads = pack_slabs(arrays)
    slabs = (
        lax.ppermute(tails, "gx", ring_pairs(count_x, 1)),
        lax.ppermute(heads, "gx", ring_pairs(count_x, -1)),
    )

    def along_y(pair):
        up, down = pair
        return (
            lax.ppermute(up, "gy", ring_pairs(count_y, 1)),
            lax.ppermute(down, "gy", ring_pairs(count_y, -1)),
        )

    strips = along_y(pack_own(arrays))
    corners = along_y(pack_corners(slabs, extent_x))
    halos = [in_vmem(a) for a in (*slabs, *strips, *corners)]
    shape = (extent_x + 2 * REACH, extent_y + 2 * TILE, LANES)
    row, *fields = pl.pallas_call(
        before_kernel,
        in_specs=[leave] * 3 + [vmem] * 6,
        out_specs=[vmem] * 9,
        out_shape=[vmem_result((count_y, LANES))] + [vmem_result(shape)] * 8,
        scratch_shapes=[vmem_array(shape)] * 3 + [pltpu.SemaphoreType.DMA((3,))],
        compiler_params=limits,
        name="smooth_before",
    )(*arrays, *halos)
    rows = add_rows(spread(row, "gy", list(range(count_y))), count_x)
    half = count_x // 2
    order = list(range(half, count_x)) + list(range(half))
    packed = spread(rows, "gx", order)
    turn = SIDE // TILE // 2
    if count_x != SIDE:
        packed = jnp.pad(jnp.roll(packed, half, 0), ((0, SIDE - count_x), (0, 0)))
        turn = 0
    return pl.pallas_call(
        after_kernel(turn, (count_x, count_y)),
        in_specs=[vmem] * 9,
        out_specs=leave,
        out_shape=jax.ShapeDtypeStruct(conductivity.shape, jnp.float32),
        scratch_shapes=[vmem_array(shape)] * 3
        + [vmem_array(conductivity.shape), pltpu.SemaphoreType.DMA((extent_x // 8,))],
        compiler_params=limits,
        name="smooth_after",
    )(*map(in_vmem, (packed, *fields)))


def solution(mesh):
    return jax.shard_map(
        body,
        mesh=mesh,
        in_specs=(P("gx", "gy", None), P("gx", "gy", None), P("gx", "gy", None)),
        out_specs=P("gx", "gy", None),
        check_vma=False,
    )
```

```python
import jax
import jax.numpy as jnp
from jax import lax
from jax.experimental import pallas as pl
from jax.experimental.pallas import tpu as pltpu
from jax.sharding import PartitionSpec as P

NU = 3
CG_ITERS = 32


relax_weight = 0.8
REACH = 2 * NU
WIDTHS = (REACH, REACH - 1, REACH)
LANES = 128
TILE = 8
SIDE = 32


def ring_pairs(count, step):
    return [(i, i + step) for i in range(count) if 0 <= i + step < count]


def own_rows():
    return [(array, row) for array, width in enumerate(WIDTHS) for row in range(width)]


def corner_rows():
    return [
        (array, beyond, width - beyond)
        for array, width in enumerate(WIDTHS)
        for beyond in range(1, width)
    ]


def vmem_array(shape):
    return pltpu.VMEM(shape, jnp.float32)


def vmem_result(shape):
    return vmem_array(shape)


def in_vmem(array):
    return pltpu.with_memory_space_constraint(array, pltpu.VMEM)


def in_hbm(array):
    return pltpu.with_memory_space_constraint(array, pltpu.HBM)


vmem = pl.BlockSpec(memory_space=pltpu.VMEM)
leave = pl.BlockSpec(memory_space=pl.ANY)
limits = pltpu.CompilerParams(vmem_limit_bytes=24 * 2**20)


def pack_edges(arrays):
    extent_x, extent_y = arrays[0].shape[:2]
    starts = (0, WIDTHS[0], WIDTHS[0] + WIDTHS[1])
    slab = (sum(WIDTHS), *arrays[0].shape[1:])
    strip = (extent_x * len(own_rows()), LANES)

    def kernel(*refs):
        refs, (up, down, tails, heads), edges, sems = refs[:3], refs[3:7], refs[7:13], refs[13]
        pairs = []
        for k, ref in enumerate(refs):
            pairs.append((ref.at[:, pl.ds(0, TILE)], edges[k]))
            pairs.append((ref.at[:, pl.ds(extent_y - TILE, TILE)], edges[3 + k]))
        for ref, width, at in zip(refs, WIDTHS, starts):
            pairs.append((ref.at[pl.ds(extent_x - width, width)], tails.at[pl.ds(at, width)]))
            pairs.append((ref.at[pl.ds(0, width)], heads.at[pl.ds(at, width)]))
        copies = start_copies(pairs, sems)
        for copy in copies[:6]:
            copy.wait()
        for k, (array, row) in enumerate(own_rows()):
            rows = slice(k * extent_x, (k + 1) * extent_x)
            up[rows, :] = edges[3 + array][:, TILE - WIDTHS[array] + row, :]
            down[rows, :] = edges[array][:, row, :]
        for copy in copies[6:]:
            copy.wait()

    results = pl.pallas_call(
        kernel,
        in_specs=[leave] * 3,
        out_specs=[vmem] * 4,
        out_shape=[vmem_result(strip)] * 2 + [vmem_result(slab)] * 2,
        scratch_shapes=[vmem_array((extent_x, TILE, LANES))] * 6
        + [pltpu.SemaphoreType.DMA((12,))],
        compiler_params=limits,
        name="pack_edges",
    )(*map(in_hbm, arrays))
    return results[:2], results[2:]


def pack_corners(strips, extent_x):
    length = 2 * sum(rows for _, _, rows in corner_rows())

    def kernel(low_ref, high_ref, up_ref, down_ref):
        at = 0
        for array, beyond, rows in corner_rows():
            first = sum(WIDTHS[:array])
            low = (first + WIDTHS[array] - rows) * extent_x
            high = first * extent_x
            for ref, start in ((low_ref, low), (high_ref, high)):
                for k in range(rows):
                    line = start + k * extent_x
                    last = line + extent_x - beyond
                    up_ref[at : at + 1, :] = ref[last : last + 1, :]
                    down_ref[at : at + 1, :] = ref[line + beyond - 1 : line + beyond, :]
                    at += 1

    return pl.pallas_call(
        kernel,
        in_specs=[vmem] * 2,
        out_specs=[vmem] * 2,
        out_shape=[vmem_result((length, LANES))] * 2,
        compiler_params=limits,
        name="pack_corners",
    )(*map(in_vmem, strips))


def plane_rolls(values, axis):
    return pltpu.roll(values, values.shape[axis] - 1, axis), pltpu.roll(values, 1, axis)


def coefficients(cond, cond_next, face_west):
    lane = lax.broadcasted_iota(jnp.int32, cond.shape, 1)
    cond_up, cond_down = plane_rolls(cond, 1)
    face_east = 0.5 * (cond + cond_next)
    face_north = 0.5 * (cond + plane_rolls(cond, 0)[0])
    face_south = plane_rolls(face_north, 0)[1]
    face_up = jnp.where(lane < LANES - 1, 0.5 * (cond + cond_up), 0.0)
    face_down = jnp.where(lane > 0, 0.5 * (cond + cond_down), 0.0)
    diagonal = (face_east + face_west) + (face_north + face_south) + (face_up + face_down)
    scale = jnp.where(cond > 0, relax_weight / diagonal, 0.0)
    return face_east, face_north, face_south, face_up, face_down, scale


def prepare(first, size, cond_ref, face_refs, face_west):
    limit = cond_ref.shape[0] - 1
    for k in range(size):
        plane = first + k
        made = coefficients(cond_ref[plane], cond_ref[jnp.minimum(plane + 1, limit)], face_west)
        for ref, part in zip(face_refs, made):
            ref[plane] = part
        face_west = made[0]
    return face_west


def sweep(low, count, size, value_ref, source_ref, face_refs, store, rows=slice(None)):
    face_x, face_n, face_s, face_u, face_d, scales = face_refs

    def block(index, carried):
        before, value, face_west = carried
        for k in range(size):
            plane = low + index * size + k
            value_next = value_ref[plane + 1]
            face_east = face_x[plane, rows]
            north, south = plane_rolls(value, 0)
            up, down = plane_rolls(value[rows], 1)
            near = (face_east * value_next[rows] + face_west * before) + (
                face_n[plane, rows] * north[rows] + face_s[plane, rows] * south[rows]
            )
            near = near + (face_u[plane, rows] * up + face_d[plane, rows] * down)
            value_own = value[rows]
            result = (1.0 - relax_weight) * value_own + scales[plane, rows] * (
                near + source_ref[plane, rows]
            )
            store(index, k, plane, result)
            before, value, face_west = value_own, value_next, face_east
        return before, value, face_west

    start = (value_ref[low - 1, rows], value_ref[low], face_x[low - 1, rows])
    lax.fori_loop(0, count // size, block, start)


def keep_in(ref):
    def store(index, k, plane, value):
        ref[plane] = value

    return store


def start_copies(pairs, sems):
    copies = [pltpu.make_async_copy(a, b, sems.at[k]) for k, (a, b) in enumerate(pairs)]
    for copy in copies:
        copy.start()
    return copies


def own_part(ext, extent_x, extent_y):
    return ext.at[pl.ds(REACH, extent_x), pl.ds(TILE, extent_y)]


def place_halos(ext_refs, slab_refs, strip_refs, corner_refs, extent_x, extent_y):
    inner = slice(TILE, TILE + extent_y)
    for ext, width, start in zip(ext_refs, WIDTHS, (0, WIDTHS[0], WIDTHS[0] + WIDTHS[1])):
        planes = ext.shape[0]
        zeros = jnp.zeros((planes, TILE, LANES), jnp.float32)
        ext[:, 0:TILE, :] = zeros
        ext[:, TILE + extent_y : 2 * TILE + extent_y, :] = zeros
        for plane in range(REACH - width):
            for side in (plane, planes - 1 - plane):
                ext[side, inner, :] = jnp.zeros((extent_y, LANES), jnp.float32)
        part = slice(start, start + width)
        ext[REACH - width : REACH, inner, :] = slab_refs[0][part]
        ext[REACH + extent_x : REACH + extent_x + width, inner, :] = slab_refs[1][part]
    for k, (array, row) in enumerate(own_rows()):
        ext, rows = ext_refs[array], slice(k * extent_x, (k + 1) * extent_x)
        own = slice(REACH, REACH + extent_x)
        ext[own, TILE - WIDTHS[array] + row, :] = strip_refs[0][rows, :]
        ext[own, TILE + extent_y + row, :] = strip_refs[1][rows, :]
    at = 0
    for array, beyond, rows in corner_rows():
        ext = ext_refs[array]
        for plane, ref in zip((REACH - beyond, REACH + extent_x - 1 + beyond), corner_refs):
            ext[plane, TILE - rows : TILE, :] = ref[at : at + rows, :]
            edge = TILE + extent_y
            ext[plane, edge : edge + rows, :] = ref[at + rows : at + 2 * rows, :]
        at += 2 * rows


def before_kernel(
    cond_in, source_in, value_in, slab_low, slab_high, strip_low, strip_high, corner_low,
    corner_high, row_ref, other, source_ext, face_x, face_n, face_s, face_u, face_d, scales,
    cond_ext, value_ext, sems,
):
    extent_x, extent_y = cond_in.shape[0], cond_in.shape[1]
    planes = extent_x + 2 * REACH
    exts = (cond_ext, source_ext, value_ext)
    face_refs = (face_x, face_n, face_s, face_u, face_d, scales)
    pairs = [
        (ref, own_part(ext, extent_x, extent_y))
        for ref, ext in zip((cond_in, source_in, value_in), exts)
    ]
    copies = start_copies(pairs, sems)
    place_halos(
        exts,
        (slab_low, slab_high),
        (strip_low, strip_high),
        (corner_low, corner_high),
        extent_x,
        extent_y,
    )
    blank = jnp.zeros(cond_ext.shape[1:], jnp.float32)
    other[0] = blank
    other[planes - 1] = blank
    for copy in copies:
        copy.wait()

    def prepare_block(index, face_west):
        return prepare(11 * index, 11, cond_ext, face_refs, face_west)

    lax.fori_loop(0, planes // 11, prepare_block, blank)
    shared = (source_ext, face_refs)
    sweep(1, planes - 2, 21, value_ext, *shared, keep_in(other))
    sweep(1, planes - 2, 21, other, *shared, keep_in(value_ext))
    sweep(1, planes - 2, 21, value_ext, *shared, keep_in(other))

    inner = slice(TILE, TILE + extent_y)
    low_x, high_x = REACH, REACH + extent_x - 1
    east = face_x[high_x, inner, :]
    west = face_x[low_x - 1, inner, :]
    net = east * (other[high_x + 1, inner, :] - other[high_x, inner, :]) + west * (
        other[low_x - 1, inner, :] - other[low_x, inner, :]
    )
    edge_low, edge_high = slice(0, 2 * TILE), slice(extent_y, extent_y + 2 * TILE)
    zero = jnp.zeros((extent_y, LANES), jnp.float32)
    zero_edge = jnp.zeros((2 * TILE, LANES), jnp.float32)

    def along(index, carried):
        sources, flow_low, flow_high, face_low, face_high = carried
        for k in range(4):
            plane = low_x + 4 * index + k
            sources = sources + source_ext[plane, inner, :]
            value = other[plane, edge_low, :]
            face = face_n[plane, edge_low, :]
            flow_low = flow_low + face * (plane_rolls(value, 0)[0] - value)
            face_low = face_low + face
            value = other[plane, edge_high, :]
            face = face_n[plane, edge_high, :]
            flow_high = flow_high + face * (plane_rolls(value, 0)[0] - value)
            face_high = face_high + face
        return sources, flow_low, flow_high, face_low, face_high

    sources, flow_low, flow_high, face_low, face_high = lax.fori_loop(
        0, extent_x // 4, along, (zero, zero_edge, zero_edge, zero_edge, zero_edge)
    )
    edge_row = lax.broadcasted_iota(jnp.int32, zero_edge.shape, 0) == TILE - 1

    def whole(values):
        return jnp.sum(jnp.sum(values, axis=0, keepdims=True), axis=1, keepdims=True)

    def face_sum(values):
        return whole(jnp.where(edge_row, values, 0.0))

    flow_north, flow_south = face_sum(face_high), face_sum(face_low)
    flow_east, flow_west = whole(east), whole(west)
    residual = whole(sources + net) + (face_sum(flow_high) - face_sum(flow_low))
    diag = flow_east + flow_west + flow_north + flow_south
    place = lax.broadcasted_iota(jnp.int32, row_ref.shape, 1) - lax.axis_index("gy")
    row = jnp.where(place == 3 * SIDE, flow_north, 0.0)
    row = jnp.where(place == 2 * SIDE, flow_east, row)
    row = jnp.where(place == SIDE, diag, row)
    row_ref[...] = jnp.where(place == 0, residual, row)


def total(values):
    return jnp.sum(jnp.sum(values, axis=1, keepdims=True), axis=0, keepdims=True)


def brick_index(shape):
    sublane = lax.broadcasted_iota(jnp.int32, shape, 0)
    lane = lax.broadcasted_iota(jnp.int32, shape, 1)
    return lane // SIDE * TILE + sublane, lane % SIDE


def fold(packed_ref, turn, part):
    lane = lax.broadcasted_iota(jnp.int32, (TILE, LANES), 1)
    folded = jnp.zeros((TILE, LANES), jnp.float32)
    for group in range(LANES // SIDE):
        start = (group + turn) % (SIDE // TILE) * TILE
        rows = packed_ref[start : start + TILE, :]
        shift = SIDE * (group - part) % LANES
        rows = pltpu.roll(rows, shift, 1) if shift else rows
        folded = jnp.where(lane // SIDE == group, rows, folded)
    return folded


def around(values):
    sublane = lax.broadcasted_iota(jnp.int32, values.shape, 0)
    ahead, behind = plane_rolls(values, 0)
    return (
        jnp.where(sublane == TILE - 1, pltpu.roll(ahead, LANES - SIDE, 1), ahead),
        jnp.where(sublane == 0, pltpu.roll(behind, SIDE, 1), behind),
        pltpu.roll(values, LANES - 1, 1),
        pltpu.roll(values, 1, 1),
    )


def coarse_solver(packed_ref, turn, count_x, count_y):
    start, diag, east, north = (fold(packed_ref, turn, part) for part in range(4))
    brick_x, brick_y = brick_index(start.shape)
    east = jnp.where(brick_x < count_x - 1, east, 0.0)
    north = jnp.where(brick_y < count_y - 1, north, 0.0)
    west, south = around(east)[1], around(north)[3]

    def products(remainder, beside):
        image = (
            diag * remainder
            - (east * beside[0] + west * beside[1])
            - (north * beside[2] + south * beside[3])
        )
        return image, around(image), total(remainder * remainder), total(image * remainder)

    def moved(state, alpha, norm, search, image, image_beside):
        estimate, remainder, beside = state
        estimate = estimate + alpha * search
        remainder = remainder - alpha * image
        beside = tuple(b - alpha * i for b, i in zip(beside, image_beside))
        return estimate, remainder, beside, search, image, image_beside, norm, alpha

    beside = around(start)
    image, image_beside, norm, curve = products(start, beside)
    first = moved(
        (jnp.zeros_like(start), start, beside), norm / curve, norm, start, image, image_beside
    )

    def iterate_once(carried):
        estimate, remainder, beside, search, image, image_beside, norm_before, alpha = carried
        new_image, new_beside, norm, curve = products(remainder, beside)
        beta = norm / norm_before
        alpha = norm / (curve - beta * norm / alpha)
        search = remainder + beta * search
        image = new_image + beta * image
        image_beside = tuple(n + beta * i for n, i in zip(new_beside, image_beside))
        return moved(
            (estimate, remainder, beside), alpha, norm, search, image, image_beside
        )

    return first, iterate_once


def after_kernel(turn, counts):
    def kernel(
        packed_ref, value_in, source_ext, face_x, face_n, face_s, face_u, face_d, scales, out_ref,
        value_ext, other, out_part, out_sems,
    ):
        extent_x, extent_y = out_ref.shape[0], out_ref.shape[1]
        planes = extent_x + 2 * REACH
        face_refs = (face_x, face_n, face_s, face_u, face_d, scales)
        low = NU + 1
        state, iterate_once = coarse_solver(packed_ref, turn, *counts)
        state = lax.fori_loop(0, CG_ITERS - 1, lambda i, s: iterate_once(s), state)
        estimate = state[0]

        brick_x, brick_y = brick_index(estimate.shape)
        step_x = brick_x - lax.axis_index("gx")
        step_y = brick_y - lax.axis_index("gy")
        row = lax.broadcasted_iota(jnp.int32, value_in.shape[1:], 0)

        def lift_of(step):
            low, own, high = (
                total(jnp.where((step_x == step) & (step_y == side), estimate, 0.0))
                for side in (-1, 0, 1)
            )
            return jnp.where(row < TILE, low, jnp.where(row < TILE + extent_y, own, high))

        lifts = [lift_of(step) for step in (-1, 0, 1)]

        def lift(plane, amount):
            inside = scales[plane] > 0
            value_ext[plane] = value_in[plane] + jnp.where(inside, amount, 0.0)

        for k in range(NU):
            lift(NU + k, lifts[0])
            lift(REACH + extent_x + k, lifts[2])

        def lift_block(index, carried):
            for k in range(4):
                lift(REACH + 4 * index + k, lifts[1])
            return carried

        lax.fori_loop(0, extent_x // 4, lift_block, 0)

        shared = (source_ext, face_refs)
        sweep(low, planes - 2 * low, 18, value_ext, *shared, keep_in(other))
        sweep(low + 1, planes - 2 * low, 18, other, *shared, keep_in(value_ext))
        size = 16

        def part(index):
            rows = pl.ds(index * size, size)
            return pltpu.make_async_copy(out_part.at[rows], out_ref.at[rows], out_sems.at[index])

        def finish(index, k, plane, value):
            out_part[index * size + k] = value
            if k == size - 1:
                part(index).start()

        inner = slice(TILE, TILE + extent_y)
        sweep(REACH, extent_x, size, value_ext, *shared, finish, inner)
        for index in range(extent_x // size):
            part(index).wait()

    return kernel


def add_rows(gathered, count):
    def kernel(rows_ref, out_ref):
        row = jnp.sum(rows_ref[...], axis=0, keepdims=True)
        out_ref[...] = jnp.broadcast_to(row, out_ref.shape)

    return pl.pallas_call(
        kernel,
        in_specs=[vmem],
        out_specs=vmem,
        out_shape=vmem_result((count, LANES)),
        compiler_params=pltpu.CompilerParams(vmem_limit_bytes=2**20),
        name="add_rows",
    )(in_vmem(gathered))


def spread(rows, axis, order):
    return lax.all_to_all(rows, axis, 0, 0, tiled=True, axis_index_groups=[order])


def body(conductivity, source, initial):
    arrays = (conductivity, source, initial)
    extent_x, extent_y = conductivity.shape[:2]
    count_x, count_y = lax.axis_size("gx"), lax.axis_size("gy")
    def along(axis, count, pair):
        up, down = pair
        return (
            lax.ppermute(up, axis, ring_pairs(count, 1)),
            lax.ppermute(down, axis, ring_pairs(count, -1)),
        )

    strips, slabs = pack_edges(arrays)
    strips = along("gy", count_y, strips)
    slabs = along("gx", count_x, slabs)
    corners = along("gx", count_x, pack_corners(strips, extent_x))
    halos = [in_vmem(a) for a in (*slabs, *strips, *corners)]
    shape = (extent_x + 2 * REACH, extent_y + 2 * TILE, LANES)
    row, *fields = pl.pallas_call(
        before_kernel,
        in_specs=[leave] * 3 + [vmem] * 6,
        out_specs=[vmem] * 9,
        out_shape=[vmem_result((count_y, LANES))] + [vmem_result(shape)] * 8,
        scratch_shapes=[vmem_array(shape)] * 2 + [pltpu.SemaphoreType.DMA((3,))],
        compiler_params=limits,
        name="smooth_before",
    )(*arrays, *halos)
    start = count_y // 3 + 1
    order = [start, *(y for y in range(count_y) if y != start)]
    rows = add_rows(spread(row, "gy", order), count_x)
    half = count_x // 2
    order = list(range(half, count_x)) + list(range(half))
    packed = spread(rows, "gx", order)
    turn = SIDE // TILE // 2
    if count_x != SIDE:
        packed = jnp.pad(jnp.roll(packed, half, 0), ((0, SIDE - count_x), (0, 0)))
        turn = 0
    return pl.pallas_call(
        after_kernel(turn, (count_x, count_y)),
        in_specs=[vmem] * 9,
        out_specs=leave,
        out_shape=jax.ShapeDtypeStruct(conductivity.shape, jnp.float32),
        scratch_shapes=[vmem_array(shape)] * 2
        + [vmem_array(conductivity.shape), pltpu.SemaphoreType.DMA((extent_x // 16,))],
        compiler_params=limits,
        name="smooth_after",
    )(*map(in_vmem, (packed, *fields)))


def solution(mesh):
    return jax.shard_map(
        body,
        mesh=mesh,
        in_specs=(P("gx", "gy", None), P("gx", "gy", None), P("gx", "gy", None)),
        out_specs=P("gx", "gy", None),
        check_vma=False,
    )
```

```python
import jax
import jax.numpy as jnp
from jax import lax
from jax.experimental import pallas as pl
from jax.experimental.pallas import tpu as pltpu
from jax.sharding import PartitionSpec as P

NU = 3
CG_ITERS = 32


relax_weight = 0.8
REACH = 2 * NU
WIDTHS = (REACH, REACH - 1, REACH)
LANES = 128
TILE = 8
SIDE = 32


def ring_pairs(count, step):
    return [(i, i + step) for i in range(count) if 0 <= i + step < count]


def own_rows(extent_x):
    rows, at = [], 0
    for array, width in enumerate(WIDTHS):
        for plane in range(extent_x):
            rows.append((array, plane, at))
            at += width
    return rows


def corner_rows():
    return [
        (array, beyond, width - beyond)
        for array, width in enumerate(WIDTHS)
        for beyond in range(1, width)
    ]


def vmem_array(shape):
    return pltpu.VMEM(shape, jnp.float32)


def vmem_result(shape):
    return vmem_array(shape)


def in_vmem(array):
    return pltpu.with_memory_space_constraint(array, pltpu.VMEM)


def in_hbm(array):
    return pltpu.with_memory_space_constraint(array, pltpu.HBM)


vmem = pl.BlockSpec(memory_space=pltpu.VMEM)
leave = pl.BlockSpec(memory_space=pl.ANY)
limits = pltpu.CompilerParams(vmem_limit_bytes=24 * 2**20)


def pack_edges(arrays):
    extent_x, extent_y = arrays[0].shape[:2]
    starts = (0, WIDTHS[0], WIDTHS[0] + WIDTHS[1])
    slab = (sum(WIDTHS), *arrays[0].shape[1:])
    strip = (extent_x * sum(WIDTHS), LANES)

    def kernel(*refs):
        refs, (up, down, tails, heads), edges, sems = refs[:3], refs[3:7], refs[7:13], refs[13]
        pairs = []
        for k, ref in enumerate(refs):
            pairs.append((ref.at[:, pl.ds(0, TILE)], edges[k]))
            pairs.append((ref.at[:, pl.ds(extent_y - TILE, TILE)], edges[3 + k]))
        for ref, width, at in zip(refs, WIDTHS, starts):
            pairs.append((ref.at[pl.ds(extent_x - width, width)], tails.at[pl.ds(at, width)]))
            pairs.append((ref.at[pl.ds(0, width)], heads.at[pl.ds(at, width)]))
        copies = start_copies(pairs, sems)
        for copy in copies[:6]:
            copy.wait()
        for array, plane, at in own_rows(extent_x):
            width = WIDTHS[array]
            up[at : at + width, :] = edges[3 + array][plane, TILE - width : TILE, :]
            down[at : at + width, :] = edges[array][plane, 0:width, :]
        for copy in copies[6:]:
            copy.wait()

    results = pl.pallas_call(
        kernel,
        in_specs=[leave] * 3,
        out_specs=[vmem] * 4,
        out_shape=[vmem_result(strip)] * 2 + [vmem_result(slab)] * 2,
        scratch_shapes=[vmem_array((extent_x, TILE, LANES))] * 6
        + [pltpu.SemaphoreType.DMA((12,))],
        compiler_params=limits,
        name="pack_edges",
    )(*map(in_hbm, arrays))
    return results[:2], results[2:]


def pack_corners(strips, extent_x):
    length = 2 * sum(rows for _, _, rows in corner_rows())

    def kernel(low_ref, high_ref, up_ref, down_ref):
        at = 0
        for array, beyond, rows in corner_rows():
            width = WIDTHS[array]
            first = sum(WIDTHS[:array]) * extent_x
            for out, plane in ((up_ref, extent_x - beyond), (down_ref, beyond - 1)):
                start = first + plane * width
                out[at : at + rows, :] = low_ref[start + width - rows : start + width, :]
                out[at + rows : at + 2 * rows, :] = high_ref[start : start + rows, :]
            at += 2 * rows

    return pl.pallas_call(
        kernel,
        in_specs=[vmem] * 2,
        out_specs=[vmem] * 2,
        out_shape=[vmem_result((length, LANES))] * 2,
        compiler_params=limits,
        name="pack_corners",
    )(*map(in_vmem, strips))


def plane_rolls(values, axis):
    return pltpu.roll(values, values.shape[axis] - 1, axis), pltpu.roll(values, 1, axis)


def coefficients(cond, cond_next, face_west):
    lane = lax.broadcasted_iota(jnp.int32, cond.shape, 1)
    cond_up, cond_down = plane_rolls(cond, 1)
    face_east = 0.5 * (cond + cond_next)
    face_north = 0.5 * (cond + plane_rolls(cond, 0)[0])
    face_south = plane_rolls(face_north, 0)[1]
    face_up = jnp.where(lane < LANES - 1, 0.5 * (cond + cond_up), 0.0)
    face_down = jnp.where(lane > 0, 0.5 * (cond + cond_down), 0.0)
    diagonal = (face_east + face_west) + (face_north + face_south) + (face_up + face_down)
    scale = jnp.where(cond > 0, relax_weight / diagonal, 0.0)
    return face_east, face_north, face_south, face_up, face_down, scale


def prepare(first, size, cond_ref, face_refs, face_west):
    limit = cond_ref.shape[0] - 1
    for k in range(size):
        plane = first + k
        made = coefficients(cond_ref[plane], cond_ref[jnp.minimum(plane + 1, limit)], face_west)
        for ref, part in zip(face_refs, made):
            ref[plane] = part
        face_west = made[0]
    return face_west


def sweep(low, count, size, value_ref, source_ref, face_refs, store, rows=slice(None)):
    face_x, face_n, face_s, face_u, face_d, scales = face_refs

    def block(index, carried):
        before, value, face_west = carried
        for k in range(size):
            plane = low + index * size + k
            value_next = value_ref[plane + 1]
            face_east = face_x[plane, rows]
            north, south = plane_rolls(value, 0)
            up, down = plane_rolls(value[rows], 1)
            near = (face_east * value_next[rows] + face_west * before) + (
                face_n[plane, rows] * north[rows] + face_s[plane, rows] * south[rows]
            )
            near = near + (face_u[plane, rows] * up + face_d[plane, rows] * down)
            value_own = value[rows]
            result = (1.0 - relax_weight) * value_own + scales[plane, rows] * (
                near + source_ref[plane, rows]
            )
            store(index, k, plane, result)
            before, value, face_west = value_own, value_next, face_east
        return before, value, face_west

    start = (value_ref[low - 1, rows], value_ref[low], face_x[low - 1, rows])
    lax.fori_loop(0, count // size, block, start)


def keep_in(ref):
    def store(index, k, plane, value):
        ref[plane] = value

    return store


def start_copies(pairs, sems):
    copies = [pltpu.make_async_copy(a, b, sems.at[k]) for k, (a, b) in enumerate(pairs)]
    for copy in copies:
        copy.start()
    return copies


def own_part(ext, extent_x, extent_y):
    return ext.at[pl.ds(REACH, extent_x), pl.ds(TILE, extent_y)]


def place_halos(ext_refs, slab_refs, strip_refs, corner_refs, extent_x, extent_y):
    inner = slice(TILE, TILE + extent_y)
    for ext, width, start in zip(ext_refs, WIDTHS, (0, WIDTHS[0], WIDTHS[0] + WIDTHS[1])):
        planes = ext.shape[0]
        zeros = jnp.zeros((planes, TILE, LANES), jnp.float32)
        ext[:, 0:TILE, :] = zeros
        ext[:, TILE + extent_y : 2 * TILE + extent_y, :] = zeros
        for plane in range(REACH - width):
            for side in (plane, planes - 1 - plane):
                ext[side, inner, :] = jnp.zeros((extent_y, LANES), jnp.float32)
        part = slice(start, start + width)
        ext[REACH - width : REACH, inner, :] = slab_refs[0][part]
        ext[REACH + extent_x : REACH + extent_x + width, inner, :] = slab_refs[1][part]
    edge = TILE + extent_y
    for array, plane, at in own_rows(extent_x):
        ext, width = ext_refs[array], WIDTHS[array]
        ext[REACH + plane, TILE - width : TILE, :] = strip_refs[0][at : at + width, :]
        ext[REACH + plane, edge : edge + width, :] = strip_refs[1][at : at + width, :]
    at = 0
    for array, beyond, rows in corner_rows():
        ext = ext_refs[array]
        for plane, ref in zip((REACH - beyond, REACH + extent_x - 1 + beyond), corner_refs):
            ext[plane, TILE - rows : TILE, :] = ref[at : at + rows, :]
            ext[plane, edge : edge + rows, :] = ref[at + rows : at + 2 * rows, :]
        at += 2 * rows


def before_kernel(
    cond_in, source_in, value_in, slab_low, slab_high, strip_low, strip_high, corner_low,
    corner_high, row_ref, other, source_ext, face_x, face_n, face_s, face_u, face_d, scales,
    cond_ext, value_ext, sems,
):
    extent_x, extent_y = cond_in.shape[0], cond_in.shape[1]
    planes = extent_x + 2 * REACH
    exts = (cond_ext, source_ext, value_ext)
    face_refs = (face_x, face_n, face_s, face_u, face_d, scales)
    pairs = [
        (ref, own_part(ext, extent_x, extent_y))
        for ref, ext in zip((cond_in, source_in, value_in), exts)
    ]
    copies = start_copies(pairs, sems)
    place_halos(
        exts,
        (slab_low, slab_high),
        (strip_low, strip_high),
        (corner_low, corner_high),
        extent_x,
        extent_y,
    )
    blank = jnp.zeros(cond_ext.shape[1:], jnp.float32)
    for copy in copies:
        copy.wait()

    def prepare_block(index, face_west):
        return prepare(11 * index, 11, cond_ext, face_refs, face_west)

    lax.fori_loop(0, planes // 11, prepare_block, blank)
    shared = (source_ext, face_refs)
    sweep(1, planes - 2, planes // 2 - 1, value_ext, *shared, keep_in(other))
    sweep(2, planes - 4, planes // 2 - 2, other, *shared, keep_in(value_ext))
    sweep(3, planes - 6, planes // 2 - 3, value_ext, *shared, keep_in(other))

    inner = slice(TILE, TILE + extent_y)
    low_x, high_x = REACH, REACH + extent_x - 1
    east = face_x[high_x, inner, :]
    west = face_x[low_x - 1, inner, :]
    net = east * (other[high_x + 1, inner, :] - other[high_x, inner, :]) + west * (
        other[low_x - 1, inner, :] - other[low_x, inner, :]
    )
    edge_low, edge_high = slice(0, 2 * TILE), slice(extent_y, extent_y + 2 * TILE)
    zero = jnp.zeros((extent_y, LANES), jnp.float32)
    zero_edge = jnp.zeros((2 * TILE, LANES), jnp.float32)

    def along(index, carried):
        sources, flow_low, flow_high, face_low, face_high = carried
        for k in range(4):
            plane = low_x + 4 * index + k
            sources = sources + source_ext[plane, inner, :]
            value = other[plane, edge_low, :]
            face = face_n[plane, edge_low, :]
            flow_low = flow_low + face * (plane_rolls(value, 0)[0] - value)
            face_low = face_low + face
            value = other[plane, edge_high, :]
            face = face_n[plane, edge_high, :]
            flow_high = flow_high + face * (plane_rolls(value, 0)[0] - value)
            face_high = face_high + face
        return sources, flow_low, flow_high, face_low, face_high

    sources, flow_low, flow_high, face_low, face_high = lax.fori_loop(
        0, extent_x // 4, along, (zero, zero_edge, zero_edge, zero_edge, zero_edge)
    )
    edge_row = lax.broadcasted_iota(jnp.int32, zero_edge.shape, 0) == TILE - 1

    def whole(values):
        return jnp.sum(jnp.sum(values, axis=0, keepdims=True), axis=1, keepdims=True)

    def face_sum(values):
        return whole(jnp.where(edge_row, values, 0.0))

    flow_north, flow_south = face_sum(face_high), face_sum(face_low)
    flow_east, flow_west = whole(east), whole(west)
    residual = whole(sources + net) + (face_sum(flow_high) - face_sum(flow_low))
    diag = flow_east + flow_west + flow_north + flow_south
    place = lax.broadcasted_iota(jnp.int32, row_ref.shape, 1) - lax.axis_index("gy")
    row = jnp.where(place == 3 * SIDE, flow_north, 0.0)
    row = jnp.where(place == 2 * SIDE, flow_east, row)
    row = jnp.where(place == SIDE, diag, row)
    row_ref[...] = jnp.where(place == 0, residual, row)


def total(values):
    return jnp.sum(jnp.sum(values, axis=1, keepdims=True), axis=0, keepdims=True)


def brick_index(shape):
    sublane = lax.broadcasted_iota(jnp.int32, shape, 0)
    lane = lax.broadcasted_iota(jnp.int32, shape, 1)
    return lane // SIDE * TILE + sublane, lane % SIDE


def fold(packed_ref, turn, part):
    lane = lax.broadcasted_iota(jnp.int32, (TILE, LANES), 1)
    folded = jnp.zeros((TILE, LANES), jnp.float32)
    for group in range(LANES // SIDE):
        start = (group + turn) % (SIDE // TILE) * TILE
        rows = packed_ref[start : start + TILE, :]
        shift = SIDE * (group - part) % LANES
        rows = pltpu.roll(rows, shift, 1) if shift else rows
        folded = jnp.where(lane // SIDE == group, rows, folded)
    return folded


def around(values):
    sublane = lax.broadcasted_iota(jnp.int32, values.shape, 0)
    ahead, behind = plane_rolls(values, 0)
    return (
        jnp.where(sublane == TILE - 1, pltpu.roll(ahead, LANES - SIDE, 1), ahead),
        jnp.where(sublane == 0, pltpu.roll(behind, SIDE, 1), behind),
        pltpu.roll(values, LANES - 1, 1),
        pltpu.roll(values, 1, 1),
    )


def coarse_solver(packed_ref, turn, count_x, count_y):
    start, diag, east, north = (fold(packed_ref, turn, part) for part in range(4))
    brick_x, brick_y = brick_index(start.shape)
    east = jnp.where(brick_x < count_x - 1, east, 0.0)
    north = jnp.where(brick_y < count_y - 1, north, 0.0)
    west, south = around(east)[1], around(north)[3]

    def products(remainder, beside):
        image = (
            diag * remainder
            - (east * beside[0] + west * beside[1])
            - (north * beside[2] + south * beside[3])
        )
        return image, around(image), total(remainder * remainder), total(image * remainder)

    def moved(state, alpha, norm, search, image, image_beside):
        estimate, remainder, beside = state
        estimate = estimate + alpha * search
        remainder = remainder - alpha * image
        beside = tuple(b - alpha * i for b, i in zip(beside, image_beside))
        return estimate, remainder, beside, search, image, image_beside, norm, alpha

    beside = around(start)
    image, image_beside, norm, curve = products(start, beside)
    first = moved(
        (jnp.zeros_like(start), start, beside), norm / curve, norm, start, image, image_beside
    )

    def iterate_once(carried):
        estimate, remainder, beside, search, image, image_beside, norm_before, alpha = carried
        new_image, new_beside, norm, curve = products(remainder, beside)
        beta = norm / norm_before
        alpha = norm / (curve - beta * norm / alpha)
        search = remainder + beta * search
        image = new_image + beta * image
        image_beside = tuple(n + beta * i for n, i in zip(new_beside, image_beside))
        return moved(
            (estimate, remainder, beside), alpha, norm, search, image, image_beside
        )

    return first, iterate_once


def after_kernel(turn, counts):
    def kernel(
        packed_ref, value_in, source_ext, face_x, face_n, face_s, face_u, face_d, scales, out_ref,
        value_ext, other, out_part, out_sems,
    ):
        extent_x, extent_y = out_ref.shape[0], out_ref.shape[1]
        planes = extent_x + 2 * REACH
        face_refs = (face_x, face_n, face_s, face_u, face_d, scales)
        low = NU + 1
        state, iterate_once = coarse_solver(packed_ref, turn, *counts)
        state = lax.fori_loop(0, CG_ITERS - 1, lambda i, s: iterate_once(s), state)
        estimate = state[0]

        brick_x, brick_y = brick_index(estimate.shape)
        step_x = brick_x - lax.axis_index("gx")
        step_y = brick_y - lax.axis_index("gy")
        row = lax.broadcasted_iota(jnp.int32, value_in.shape[1:], 0)

        def lift_of(step):
            low, own, high = (
                total(jnp.where((step_x == step) & (step_y == side), estimate, 0.0))
                for side in (-1, 0, 1)
            )
            return jnp.where(row < TILE, low, jnp.where(row < TILE + extent_y, own, high))

        lifts = [lift_of(step) for step in (-1, 0, 1)]

        def lift(plane, amount):
            inside = scales[plane] > 0
            value_ext[plane] = value_in[plane] + jnp.where(inside, amount, 0.0)

        for k in range(NU):
            lift(NU + k, lifts[0])
            lift(REACH + extent_x + k, lifts[2])

        def lift_block(index, carried):
            for k in range(4):
                lift(REACH + 4 * index + k, lifts[1])
            return carried

        lax.fori_loop(0, extent_x // 4, lift_block, 0)

        shared = (source_ext, face_refs)
        half = planes // 2 - low
        sweep(low, 2 * half, half, value_ext, *shared, keep_in(other))
        sweep(low + 1, 2 * half - 2, half - 1, other, *shared, keep_in(value_ext))
        size = 16

        def part(index):
            rows = pl.ds(index * size, size)
            return pltpu.make_async_copy(out_part.at[rows], out_ref.at[rows], out_sems.at[index])

        def finish(index, k, plane, value):
            out_part[index * size + k] = value
            if k == size - 1:
                part(index).start()

        inner = slice(TILE, TILE + extent_y)
        sweep(REACH, extent_x, size, value_ext, *shared, finish, inner)
        for index in range(extent_x // size):
            part(index).wait()

    return kernel


def add_rows(gathered, count):
    def kernel(rows_ref, out_ref):
        row = jnp.sum(rows_ref[...], axis=0, keepdims=True)
        out_ref[...] = jnp.broadcast_to(row, out_ref.shape)

    return pl.pallas_call(
        kernel,
        in_specs=[vmem],
        out_specs=vmem,
        out_shape=vmem_result((count, LANES)),
        compiler_params=pltpu.CompilerParams(vmem_limit_bytes=2**20),
        name="add_rows",
    )(in_vmem(gathered))


def spread(rows, axis, order):
    return lax.all_to_all(rows, axis, 0, 0, tiled=True, axis_index_groups=[order])


def body(conductivity, source, initial):
    arrays = (conductivity, source, initial)
    extent_x, extent_y = conductivity.shape[:2]
    count_x, count_y = lax.axis_size("gx"), lax.axis_size("gy")
    def along(axis, count, pair):
        up, down = pair
        return (
            lax.ppermute(up, axis, ring_pairs(count, 1)),
            lax.ppermute(down, axis, ring_pairs(count, -1)),
        )

    strips, slabs = pack_edges(arrays)
    strips = along("gy", count_y, strips)
    slabs = along("gx", count_x, slabs)
    corners = along("gx", count_x, pack_corners(strips, extent_x))
    halos = [in_vmem(a) for a in (*slabs, *strips, *corners)]
    shape = (extent_x + 2 * REACH, extent_y + 2 * TILE, LANES)
    row, *fields = pl.pallas_call(
        before_kernel,
        in_specs=[leave] * 3 + [vmem] * 6,
        out_specs=[vmem] * 9,
        out_shape=[vmem_result((count_y, LANES))] + [vmem_result(shape)] * 8,
        scratch_shapes=[vmem_array(shape)] * 2 + [pltpu.SemaphoreType.DMA((3,))],
        compiler_params=limits,
        name="smooth_before",
    )(*arrays, *halos)
    start = count_y // 3 + 1
    order = [start, *(y for y in range(count_y) if y != start)]
    rows = add_rows(spread(row, "gy", order), count_x)
    half = count_x // 2
    order = list(range(half, count_x)) + list(range(half))
    packed = spread(rows, "gx", order)
    turn = SIDE // TILE // 2
    if count_x != SIDE:
        packed = jnp.pad(jnp.roll(packed, half, 0), ((0, SIDE - count_x), (0, 0)))
        turn = 0
    return pl.pallas_call(
        after_kernel(turn, (count_x, count_y)),
        in_specs=[vmem] * 9,
        out_specs=leave,
        out_shape=jax.ShapeDtypeStruct(conductivity.shape, jnp.float32),
        scratch_shapes=[vmem_array(shape)] * 2
        + [vmem_array(conductivity.shape), pltpu.SemaphoreType.DMA((extent_x // 16,))],
        compiler_params=limits,
        name="smooth_after",
    )(*map(in_vmem, (packed, *fields)))


def solution(mesh):
    return jax.shard_map(
        body,
        mesh=mesh,
        in_specs=(P("gx", "gy", None), P("gx", "gy", None), P("gx", "gy", None)),
        out_specs=P("gx", "gy", None),
        check_vma=False,
    )
```
